32 devices in a mesh: samp: 8 (over z, core), var: 4 (over y, x).
Axes of the slice: x: 2, y: 2, z: 4, core: 2. Of those that a mesh axis runs over, the one named last changes fastest.
Arguments:
- hap_words: int32 [2, 512, 512], P(None, 'samp', 'var'), may hold values from 0 to 1073741823
- total_counts: int32 [15360, 8192], P('samp', 'var'), may hold values from 0 to 4999
- allele_one: int32 [15360, 8192], P('samp', 'var'), may hold values from 0 to 299
- allele_two: int32 [15360, 8192], P('samp', 'var'), may hold values from 0 to 299
Outputs:
- z_total: float32 [512, 8192], P('samp', 'var')
- z_allelic: float32 [512, 8192], P('samp', 'var')
The draws below stay inside these ranges and needn't reach their ends.
Inputs may be any that keep to these rules, and one draw needn't show every extreme that they name: Bit k, for k below 30, of hap_words[c, j, v] is haplotype c of sample 30 * j + k at variant v; higher bits are zero.
All inputs are finite; a program needn't handle non-finite values.
Results may differ from the reference program's by a relative error of at most 0.0003.
The reference program's roundings to bfloat16 on the way count: a program that leaves them out, or rounds other values in their place, can miss the bound.
Values sent between devices are 32-bit elements; how exact they have to be, the bound alone decides.
A program may use at most 192 MiB of HBM per device.

```python
import jax
import jax.numpy as jnp
from jax import lax

BITS = 30
GENES = 8192
SWORDS = 512
SAMPLES = 15360
VARIANTS = 512


def with_ends(array, own_key, low, high):
    longest = array.shape.index(max(array.shape))
    spots = []
    for shift in (0, 1):
        where = [jax.random.randint(jax.random.fold_in(own_key, axis), (), 0, length) for axis, length in enumerate(array.shape)]
        where[longest] = (where[longest] + shift) % array.shape[longest]
        spots.append(tuple(where))
    return array.at[spots[0]].set(low).at[spots[1]].set(high)


def setup_inputs(seed: int = 0) -> dict:
    seeds = jax.random.split(jax.random.key(seed), 5)
    hap_words = with_ends(jax.random.randint(seeds[0], (2, SWORDS, VARIANTS), 0, 2 ** BITS), jax.random.fold_in(seeds[0], 1), 0, (2 ** BITS) - 1).astype(jnp.int32)
    total_counts = with_ends(jax.random.randint(seeds[1], (SAMPLES, GENES), 0, 5000), jax.random.fold_in(seeds[1], 1), 0, 4999).astype(jnp.int32)
    allele_one = with_ends(jax.random.randint(seeds[2], (SAMPLES, GENES), 0, 300), jax.random.fold_in(seeds[2], 1), 0, 299).astype(jnp.int32)
    allele_two = with_ends(jax.random.randint(seeds[3], (SAMPLES, GENES), 0, 300), jax.random.fold_in(seeds[3], 1), 0, 299).astype(jnp.int32)
    return dict(hap_words=hap_words, total_counts=total_counts, allele_one=allele_one, allele_two=allele_two)


def unpack(packed):
    shifts = jnp.arange(BITS, dtype=jnp.int32)
    bit_table = jnp.bitwise_and(jnp.right_shift(packed[:, :, None, :], shifts[None, None, :, None]), 1)
    return bit_table.reshape(2, packed.shape[1] * BITS, packed.shape[2])

def features(total_part, one_part, two_part):
    log_total = jnp.log1p(total_part.astype(jnp.float32))
    one_plus = one_part.astype(jnp.float32) + 1.0
    two_plus = two_part.astype(jnp.float32) + 1.0
    log_ratio = jnp.log(one_plus / two_plus)
    weight = 1.0 / (1.0 / one_plus + 1.0 / two_plus)
    return (log_total, (weight * log_ratio).astype(jnp.bfloat16), weight.astype(jnp.bfloat16))

def finish(cross_total, cross_allelic, het_weight, dos_sum, dos_sq, gene_sum, gene_sq, sample_count):
    dosage_var = dos_sq - dos_sum * dos_sum / sample_count
    gene_var = gene_sq - gene_sum * gene_sum / sample_count
    covariance = cross_total - dos_sum[:, None] * gene_sum[None, :] / sample_count
    z_total = jnp.sqrt(sample_count) * covariance / jnp.sqrt((dosage_var[:, None] + 1.0) * (gene_var[None, :] + 1.0))
    z_allelic = cross_allelic / jnp.sqrt(het_weight + 1.0)
    return (z_total, z_allelic)

def reference(hap_words, total_counts, allele_one, allele_two):
    bit_table = unpack(hap_words)
    dosage = bit_table[0] + bit_table[1] - 1
    phase_diff = bit_table[0] - bit_table[1]
    dosage_f = dosage.astype(jnp.float32)
    dos_sum = lax.optimization_barrier(jnp.sum(dosage_f, axis=0))
    dos_sq = lax.optimization_barrier(jnp.sum(dosage_f * dosage_f, axis=0))
    dosage_b = dosage.astype(jnp.bfloat16)
    phase_b = phase_diff.astype(jnp.bfloat16)
    phase_sq_b = (phase_diff * phase_diff).astype(jnp.bfloat16)
    sample_count = jnp.float32(hap_words.shape[1] * BITS)
    block_width = GENES // 8

    def one_block(block_index):
        first_col = (block_index * block_width).astype(jnp.int32)
        total_part = lax.dynamic_slice_in_dim(total_counts, first_col, block_width, 1)
        one_part = lax.dynamic_slice_in_dim(allele_one, first_col, block_width, 1)
        two_part = lax.dynamic_slice_in_dim(allele_two, first_col, block_width, 1)
        log_total, weighted_b, weight_b = features(total_part, one_part, two_part)
        cross_total = jnp.dot(dosage_b.T, log_total.astype(jnp.bfloat16), preferred_element_type=jnp.float32)
        cross_allelic = jnp.dot(phase_b.T, weighted_b, preferred_element_type=jnp.float32)
        het_weight = jnp.dot(phase_sq_b.T, weight_b, preferred_element_type=jnp.float32)
        gene_sum = lax.optimization_barrier(jnp.sum(log_total, axis=0))
        gene_sq = lax.optimization_barrier(jnp.sum(log_total * log_total, axis=0))
        return finish(cross_total, cross_allelic, het_weight, dos_sum, dos_sq, gene_sum, gene_sq, sample_count)
    total_blocks, allelic_blocks = lax.map(one_block, jnp.arange(8, dtype=jnp.int32))
    variants = hap_words.shape[2]
    z_total = jnp.moveaxis(total_blocks, 0, 1).reshape(variants, GENES)
    z_allelic = jnp.moveaxis(allelic_blocks, 0, 1).reshape(variants, GENES)
    return (z_total, z_allelic)
```

```python
import functools
import math

import jax
import jax.numpy as jnp
from jax import lax
from jax.experimental import pallas as pl
from jax.experimental.pallas import tpu as pltpu
from jax.sharding import PartitionSpec as P

BITS = 30
TILE = 256
CHUNK = 128
MESH = pl.DeviceIdType.MESH


def kernel(
    chips,
    owners,
    early,
    hap_ref,
    total_ref,
    one_ref,
    two_ref,
    z_total_ref,
    z_allelic_ref,
    words,
    nat,
    tables,
    inputs,
    feats,
    own,
    swapped,
    arrived,
    margins,
    word_send,
    word_recv,
    word_local,
    in_sem,
    swap_send,
    swap_recv,
    hop_send,
    hop_recv,
    margin_send,
    margin_recv,
):
    me = lax.axis_index("samp")
    group = lax.axis_index("var")
    place = lax.div(me, 2)
    core = lax.rem(me, 2)
    partner = me + 1 - 2 * core
    word_rows, block = words.shape[2], words.shape[3]
    samples = tables.shape[2]
    tiles = own.shape[0]
    rows = own.shape[4]
    sample_count = float(samples * 2 * chips)

    def fetch(tile, slot):
        columns = pl.ds(pl.multiple_of(tile * TILE, TILE), TILE)
        return [
            pltpu.make_async_copy(
                ref.at[:, columns], inputs.at[slot, kind], in_sem.at[slot, kind]
            )
            for kind, ref in enumerate((total_ref, one_ref, two_ref))
        ]

    for copy in fetch(0, 0):
        copy.start()
    local = pltpu.make_async_copy(hap_ref, words.at[group], word_local)
    local.start()

    barrier = pltpu.get_barrier_semaphore()
    pl.semaphore_signal(barrier, inc=1, device_id={"samp": partner}, device_id_type=MESH)

    @pl.when(place > 0)
    def _():
        pl.semaphore_signal(barrier, inc=1, device_id={"samp": me - 2}, device_id_type=MESH)

    @pl.when(place < chips - 1)
    def _():
        pl.semaphore_signal(barrier, inc=1, device_id={"samp": me + 2}, device_id_type=MESH)

    for shift in range(1, owners):
        other = lax.rem(group + shift, owners)
        pl.semaphore_signal(barrier, inc=1, device_id={"var": other}, device_id_type=MESH)
    inner = jnp.where(jnp.logical_and(place > 0, place < chips - 1), 1, 0)
    pl.semaphore_wait(barrier, owners + 1 + inner)

    def word_copy(shift):
        return pltpu.make_async_remote_copy(
            src_ref=hap_ref,
            dst_ref=words.at[group],
            send_sem=word_send.at[shift],
            recv_sem=word_recv.at[shift],
            device_id={"var": lax.rem(group + shift, owners)},
            device_id_type=MESH,
        )

    for shift in range(1, owners):
        word_copy(shift).start()

    def swap_copy(tile):
        return pltpu.make_async_remote_copy(
            src_ref=own.at[tile, :, :, 1 - core],
            dst_ref=swapped.at[tile],
            send_sem=swap_send.at[tile],
            recv_sem=swap_recv.at[tile],
            device_id={"samp": partner},
            device_id_type=MESH,
        )

    def hop_copy(tile, target, slot, toward):
        return pltpu.make_async_remote_copy(
            src_ref=arrived.at[tile, target],
            dst_ref=arrived.at[tile, slot],
            send_sem=hop_send.at[tile, target],
            recv_sem=hop_recv.at[tile, slot],
            device_id={"samp": toward},
            device_id_type=MESH,
        )

    def compute_features(tile, slot):
        def step(index, sums):
            part = pl.ds(pl.multiple_of(index * CHUNK, CHUNK), CHUNK)
            log_total = jnp.log(inputs[slot, 0, part, :].astype(jnp.float32) + 1.0)
            feats[0, part, :] = log_total.astype(jnp.bfloat16)
            one = inputs[slot, 1, part, :].astype(jnp.float32) + 1.0
            two = inputs[slot, 2, part, :].astype(jnp.float32) + 1.0
            weight = (one * two) / (one + two)
            ratio = jnp.log(one) - jnp.log(two)
            feats[1, part, :] = (weight * ratio).astype(jnp.bfloat16)
            feats[2, part, :] = weight.astype(jnp.bfloat16)
            split = log_total.reshape(CHUNK // 8, 8, TILE)
            return (sums[0] + jnp.sum(split, axis=0), sums[1] + jnp.sum(split * split, axis=0))

        zero = jnp.zeros((8, TILE), jnp.float32)
        sums = lax.fori_loop(0, samples // CHUNK, step, (zero, zero))
        margins[0, tile, 0:1, :] = jnp.sum(sums[0], axis=0, keepdims=True)
        margins[0, tile, 1:2, :] = jnp.sum(sums[1], axis=0, keepdims=True)

    def build_tables():
        def step(owner, carry):
            first, second = words[owner, 0], words[owner, 1]
            for bit in range(BITS):
                low = jnp.bitwise_and(jnp.right_shift(first, bit), 1)
                high = jnp.bitwise_and(jnp.right_shift(second, bit), 1)
                spread = pl.ds(bit, word_rows, stride=BITS)
                nat[0, spread, :] = (low + high - 1).astype(jnp.float32)
                nat[1, spread, :] = (low - high).astype(jnp.float32)
            dosage = nat[0].T
            phase = nat[1].T
            part = pl.ds(pl.multiple_of(owner * block, block), block)
            tables[0, part, :] = dosage.astype(jnp.bfloat16)
            tables[1, part, :] = phase.astype(jnp.bfloat16)
            tables[2, part, :] = (phase * phase).astype(jnp.bfloat16)
            return carry

        lax.fori_loop(0, owners, step, 0)
        per_tile = TILE // block
        for owner in range(owners):
            first, second = words[owner, 0], words[owner, 1]
            count = lax.population_count(first) + lax.population_count(second)
            differ = lax.population_count(jnp.bitwise_xor(first, second))
            lanes = pl.ds((owner % per_tile) * block, block)
            place_of = tiles + owner // per_tile
            all_bits = float(BITS * word_rows)
            margins[0, place_of, 0:1, lanes] = (
                jnp.sum(count.astype(jnp.float32), axis=0, keepdims=True) - all_bits
            )
            margins[0, place_of, 1:2, lanes] = all_bits - jnp.sum(
                differ.astype(jnp.float32), axis=0, keepdims=True
            )

    def multiply(tile):
        for kind in range(3):
            product = jnp.dot(tables[kind], feats[kind], preferred_element_type=jnp.float32)
            own[tile, kind] = product.reshape(chips, 2, rows, TILE)

    def chip_part(tile, target):
        return own[tile, :, target, core] + swapped[tile, :, target]

    def forward(tile):
        swap_copy(tile).wait_recv()
        for step in range(chips - 1):
            far, near = chips - 1 - step, step

            @pl.when(far > place)
            def _():
                @pl.when(place > 0)
                def _():
                    hop_copy(tile, far, far, me - 2).wait_recv()
                    arrived[tile, far] = arrived[tile, far] + chip_part(tile, far)

                @pl.when(place == 0)
                def _():
                    arrived[tile, far] = chip_part(tile, far)

                hop_copy(tile, far, far, me + 2).start()

            @pl.when(near < place)
            def _():
                @pl.when(place < chips - 1)
                def _():
                    hop_copy(tile, near, near, me + 2).wait_recv()
                    arrived[tile, near] = arrived[tile, near] + chip_part(tile, near)

                @pl.when(place == chips - 1)
                def _():
                    arrived[tile, near] = chip_part(tile, near)

                slot = jnp.where(place - 1 == near, chips, near)
                hop_copy(tile, near, slot, me - 2).start()

    def drain(tile):
        swap_copy(tile).wait_send()
        for target in range(chips):

            @pl.when(target != place)
            def _():
                hop_copy(tile, target, target, partner).wait_send()

    def margin_copy(index, source, slot, toward):
        return pltpu.make_async_remote_copy(
            src_ref=margins.at[source],
            dst_ref=margins.at[slot],
            send_sem=margin_send.at[index],
            recv_sem=margin_recv.at[index],
            device_id={"samp": toward},
            device_id_type=MESH,
        )

    def reduce_margins():
        margin_copy(0, 0, 1, partner).wait_recv()
        margins[2] = margins[0] + margins[1]

        @pl.when(place == 0)
        def _():
            margins[5] = margins[2]

        @pl.when(place > 0)
        def _():
            margin_copy(1, 5, 3, me - 2).wait_recv()
            margins[5] = margins[2] + margins[3]

        @pl.when(place < chips - 1)
        def _():
            margin_copy(1, 5, 3, me + 2).start()

        @pl.when(place == chips - 1)
        def _():
            margins[4] = jnp.zeros_like(margins[4])
            margins[6] = margins[2]

        @pl.when(place < chips - 1)
        def _():
            margin_copy(2, 6, 4, me + 2).wait_recv()
            margins[6] = margins[2] + margins[4]

        @pl.when(place > 0)
        def _():
            margin_copy(2, 6, 4, me - 2).start()

    def own_column(kind):
        lane = lax.broadcasted_iota(jnp.int32, (rows, TILE), 1)
        row = lax.broadcasted_iota(jnp.int32, (rows, TILE), 0)
        column = jnp.zeros((rows, 1), jnp.float32)
        for piece in range(margins.shape[1] - tiles):
            whole = (
                margins[5, tiles + piece, kind : kind + 1, :]
                + margins[4, tiles + piece, kind : kind + 1, :]
            )
            hit = lane + piece * TILE == me * rows + row
            column = column + jnp.sum(jnp.where(hit, whole, 0.0), axis=1, keepdims=True)
        return column

    def finish(tile):
        own[tile, :, place, core] = chip_part(tile, place)

        @pl.when(place > 0)
        def _():
            hop_copy(tile, place, place, me - 2).wait_recv()
            own[tile, :, place, core] = own[tile, :, place, core] + arrived[tile, place]

        @pl.when(place < chips - 1)
        def _():
            hop_copy(tile, place, chips, me + 2).wait_recv()
            own[tile, :, place, core] = own[tile, :, place, core] + arrived[tile, chips]

        sums = own[tile, :, place, core]
        dos_sum, dos_sq = own_column(0), own_column(1)
        gene_sum, gene_sq = (
            margins[5, tile, kind : kind + 1, :] + margins[4, tile, kind : kind + 1, :]
            for kind in (0, 1)
        )
        dosage_var = dos_sq - dos_sum * dos_sum / sample_count
        gene_var = gene_sq - gene_sum * gene_sum / sample_count
        covariance = sums[0] - dos_sum * gene_sum / sample_count
        columns = pl.ds(pl.multiple_of(tile * TILE, TILE), TILE)
        z_total_ref[:, columns] = (
            math.sqrt(sample_count)
            * covariance
            / jnp.sqrt((dosage_var + 1.0) * (gene_var + 1.0))
        )
        z_allelic_ref[:, columns] = sums[1] / jnp.sqrt(sums[2] + 1.0)

    for copy in fetch(0, 0):
        copy.wait()
    if tiles > 1:
        for copy in fetch(1, 1):
            copy.start()
    compute_features(0, 0)
    local.wait()
    for shift in range(1, owners):
        word_copy(shift).wait()
    build_tables()
    multiply(0)
    swap_copy(0).start()

    def compute_step(tile, carry):
        slot = lax.rem(tile, 2)
        for copy in fetch(tile, slot):
            copy.wait()

        @pl.when(tile + 1 < tiles)
        def _():
            for copy in fetch(tile + 1, 1 - slot):
                copy.start()

        compute_features(tile, slot)
        multiply(tile)
        swap_copy(tile).start()

        @pl.when(lax.rem(tile, 2) == 1)
        def _():
            ready = lax.div(tile, 2)

            @pl.when(ready < early)
            def _():
                forward(ready)

        return carry

    lax.fori_loop(1, tiles, compute_step, 0)
    margin_copy(0, 0, 1, partner).start()

    def later_step(tile, carry):
        @pl.when(tile >= 2)
        def _():
            drain(tile - 2)

        forward(tile)

        @pl.when(tile == early)
        def _():
            reduce_margins()

        @pl.when(tile > early)
        def _():
            finish(tile - 1)

        return carry

    lax.fori_loop(early, tiles, later_step, 0)
    for tile in range(early):
        finish(tile)
    finish(tiles - 1)
    for tile in range(max(early - 2, 0)):
        drain(tile)
    drain(tiles - 2)
    drain(tiles - 1)
    margin_copy(0, 0, 1, partner).wait_send()

    @pl.when(place < chips - 1)
    def _():
        margin_copy(1, 5, 3, partner).wait_send()

    @pl.when(place > 0)
    def _():
        margin_copy(2, 6, 4, partner).wait_send()


def per_device(hap_words, total_counts, allele_one, allele_two):
    devices = lax.axis_size("samp")
    owners = lax.axis_size("var")
    chips = devices // 2
    samples, genes = total_counts.shape
    _, word_rows, block = hap_words.shape
    variants = block * owners
    rows = variants // devices
    tiles = genes // TILE
    early = min(3, tiles - 2)
    pieces = variants // TILE
    hbm = pl.BlockSpec(memory_space=pltpu.MemorySpace.HBM)
    vmem = pl.BlockSpec(memory_space=pltpu.MemorySpace.VMEM)
    out = jax.ShapeDtypeStruct((rows, genes), jnp.float32)
    dma = pltpu.SemaphoreType.DMA
    f32 = jnp.float32
    return pl.pallas_call(
        functools.partial(kernel, chips, owners, early),
        out_shape=(out, out),
        in_specs=[hbm] * 4,
        out_specs=(vmem, vmem),
        scratch_shapes=[
            pltpu.VMEM((owners, 2, word_rows, block), jnp.int32),
            pltpu.VMEM((2, samples, block), f32),
            pltpu.VMEM((3, variants, samples), jnp.bfloat16),
            pltpu.VMEM((2, 3, samples, TILE), jnp.int32),
            pltpu.VMEM((3, samples, TILE), jnp.bfloat16),
            pltpu.VMEM((tiles, 3, chips, 2, rows, TILE), f32),
            pltpu.VMEM((tiles, 3, chips, rows, TILE), f32),
            pltpu.VMEM((tiles, chips + 1, 3, rows, TILE), f32),
            pltpu.VMEM((7, tiles + pieces, 2, TILE), f32),
            dma((owners,)),
            dma((owners,)),
            dma,
            dma((2, 3)),
            dma((tiles,)),
            dma((tiles,)),
            dma((tiles, chips)),
            dma((tiles, chips + 1)),
            dma((3,)),
            dma((3,)),
        ],
        compiler_params=pltpu.CompilerParams(
            collective_id=0, has_side_effects=True, vmem_limit_bytes=67043328
        ),
    )(hap_words, total_counts, allele_one, allele_two)


def solution(mesh):
    in_specs = (P(None, "samp", "var"), P("samp", "var"), P("samp", "var"), P("samp", "var"))
    out_specs = (P("samp", "var"), P("samp", "var"))
    return jax.shard_map(
        per_device, mesh=mesh, in_specs=in_specs, out_specs=out_specs, check_vma=False
    )
```

```python
import functools
import math

import jax
import jax.numpy as jnp
from jax import lax
from jax.experimental import pallas as pl
from jax.experimental.pallas import tpu as pltpu
from jax.sharding import PartitionSpec as P

BITS = 30
TILE = 256
CHUNK = 128
MESH = pl.DeviceIdType.MESH


def kernel(
    chips,
    owners,
    hap_ref,
    total_ref,
    one_ref,
    two_ref,
    z_total_ref,
    z_allelic_ref,
    words,
    nat,
    tables,
    inputs,
    feats,
    own,
    swapped,
    arrived,
    margins,
    word_send,
    word_recv,
    word_local,
    in_sem,
    swap_send,
    swap_recv,
    hop_send,
    hop_recv,
    margin_send,
    margin_recv,
):
    me = lax.axis_index("samp")
    group = lax.axis_index("var")
    place = lax.div(me, 2)
    core = lax.rem(me, 2)
    partner = me + 1 - 2 * core
    word_rows, block = words.shape[2], words.shape[3]
    samples = tables.shape[2]
    tiles = own.shape[0]
    rows = own.shape[4]
    sample_count = float(samples * 2 * chips)
    middle = jnp.logical_and(place > 0, place < chips - 1)
    left_half = place < chips // 2
    early = (tiles - 1) // 3
    meet = max(tiles - 3, 1)

    def fetch(tile, slot):
        columns = pl.ds(pl.multiple_of(tile * TILE, TILE), TILE)
        return [
            pltpu.make_async_copy(
                ref.at[:, columns], inputs.at[slot, kind], in_sem.at[slot, kind]
            )
            for kind, ref in enumerate((total_ref, one_ref, two_ref))
        ]

    for copy in fetch(0, 0):
        copy.start()
    local = pltpu.make_async_copy(hap_ref, words.at[group], word_local)
    local.start()

    barrier = pltpu.get_barrier_semaphore()
    pl.semaphore_signal(barrier, inc=1, device_id={"samp": partner}, device_id_type=MESH)

    @pl.when(place > 0)
    def _():
        pl.semaphore_signal(barrier, inc=1, device_id={"samp": me - 2}, device_id_type=MESH)

    @pl.when(place < chips - 1)
    def _():
        pl.semaphore_signal(barrier, inc=1, device_id={"samp": me + 2}, device_id_type=MESH)

    for shift in range(1, owners):
        other = lax.rem(group + shift, owners)
        pl.semaphore_signal(barrier, inc=1, device_id={"var": other}, device_id_type=MESH)
    pl.semaphore_wait(barrier, owners + 1 + jnp.where(middle, 1, 0))

    def word_copy(shift):
        return pltpu.make_async_remote_copy(
            src_ref=hap_ref,
            dst_ref=words.at[group],
            send_sem=word_send.at[shift],
            recv_sem=word_recv.at[shift],
            device_id={"var": lax.rem(group + shift, owners)},
            device_id_type=MESH,
        )

    for shift in range(1, owners):
        word_copy(shift).start()

    def swap_copy(tile):
        return pltpu.make_async_remote_copy(
            src_ref=own.at[tile, :, :, 1 - core],
            dst_ref=swapped.at[tile],
            send_sem=swap_send.at[tile],
            recv_sem=swap_recv.at[tile],
            device_id={"samp": partner},
            device_id_type=MESH,
        )

    def hop_copy(tile, target, slot, toward):
        return pltpu.make_async_remote_copy(
            src_ref=arrived.at[tile, target],
            dst_ref=arrived.at[tile, slot],
            send_sem=hop_send.at[tile, target],
            recv_sem=hop_recv.at[tile, slot],
            device_id={"samp": toward},
            device_id_type=MESH,
        )

    def compute_features(tile, slot):
        def step(index, sums):
            part = pl.ds(pl.multiple_of(index * CHUNK, CHUNK), CHUNK)
            log_total = jnp.log(inputs[slot, 0, part, :].astype(jnp.float32) + 1.0)
            feats[0, part, :] = log_total.astype(jnp.bfloat16)
            one = inputs[slot, 1, part, :].astype(jnp.float32) + 1.0
            two = inputs[slot, 2, part, :].astype(jnp.float32) + 1.0
            weight = (one * two) / (one + two)
            ratio = jnp.log(one) - jnp.log(two)
            feats[1, part, :] = (weight * ratio).astype(jnp.bfloat16)
            feats[2, part, :] = weight.astype(jnp.bfloat16)
            split = log_total.reshape(CHUNK // 8, 8, TILE)
            return (sums[0] + jnp.sum(split, axis=0), sums[1] + jnp.sum(split * split, axis=0))

        zero = jnp.zeros((8, TILE), jnp.float32)
        sums = lax.fori_loop(0, samples // CHUNK, step, (zero, zero))
        margins[0, tile, 0:1, :] = jnp.sum(sums[0], axis=0, keepdims=True)
        margins[0, tile, 1:2, :] = jnp.sum(sums[1], axis=0, keepdims=True)

    def build_tables():
        def step(owner, carry):
            first, second = words[owner, 0], words[owner, 1]
            for bit in range(BITS):
                low = jnp.bitwise_and(jnp.right_shift(first, bit), 1)
                high = jnp.bitwise_and(jnp.right_shift(second, bit), 1)
                spread = pl.ds(bit, word_rows, stride=BITS)
                nat[0, spread, :] = (low + high - 1).astype(jnp.float32)
                nat[1, spread, :] = (low - high).astype(jnp.float32)
            dosage = nat[0].T
            phase = nat[1].T
            part = pl.ds(pl.multiple_of(owner * block, block), block)
            tables[0, part, :] = dosage.astype(jnp.bfloat16)
            tables[1, part, :] = phase.astype(jnp.bfloat16)
            tables[2, part, :] = (phase * phase).astype(jnp.bfloat16)
            return carry

        lax.fori_loop(0, owners, step, 0)
        per_tile = TILE // block
        for owner in range(owners):
            first, second = words[owner, 0], words[owner, 1]
            count = lax.population_count(first) + lax.population_count(second)
            differ = lax.population_count(jnp.bitwise_xor(first, second))
            lanes = pl.ds((owner % per_tile) * block, block)
            place_of = tiles + owner // per_tile
            all_bits = float(BITS * word_rows)
            margins[0, place_of, 0:1, lanes] = (
                jnp.sum(count.astype(jnp.float32), axis=0, keepdims=True) - all_bits
            )
            margins[0, place_of, 1:2, lanes] = all_bits - jnp.sum(
                differ.astype(jnp.float32), axis=0, keepdims=True
            )

    def multiply(tile):
        for kind in range(3):
            product = jnp.dot(tables[kind], feats[kind], preferred_element_type=jnp.float32)
            own[tile, kind] = product.reshape(chips, 2, rows, TILE)

    def chip_part(tile, target):
        return own[tile, :, target, core] + swapped[tile, :, target]

    def sweep(tile, rightward):
        head = jnp.where(rightward, 0, chips - 1)
        toward = jnp.where(rightward, me + 2, me - 2)
        behind = jnp.where(rightward, me - 2, me + 2)
        for step in range(chips - 1):
            target = jnp.where(rightward, chips - 1 - step, step)
            ahead = jnp.where(rightward, target - place, place - target)

            @pl.when(ahead > 0)
            def _():
                @pl.when(place != head)
                def _():
                    hop_copy(tile, target, target, behind).wait_recv()
                    arrived[tile, target] = arrived[tile, target] + chip_part(tile, target)

                @pl.when(place == head)
                def _():
                    arrived[tile, target] = chip_part(tile, target)

                last = jnp.logical_and(jnp.logical_not(rightward), ahead == 1)
                hop_copy(tile, target, jnp.where(last, chips, target), toward).start()

    def forward(tile):
        swap_copy(tile).wait_recv()
        sweep(tile, left_half)
        sweep(tile, jnp.logical_not(left_half))

    def drain(tile):
        swap_copy(tile).wait_send()
        for target in range(chips):

            @pl.when(target != place)
            def _():
                hop_copy(tile, target, target, partner).wait_send()

    def margin_copy(index, source, slot, toward):
        return pltpu.make_async_remote_copy(
            src_ref=margins.at[source],
            dst_ref=margins.at[slot],
            send_sem=margin_send.at[index],
            recv_sem=margin_recv.at[index],
            device_id={"samp": toward},
            device_id_type=MESH,
        )

    def start_margins():
        margin_copy(0, 0, 1, partner).start()
        margin_copy(0, 0, 1, partner).wait_recv()
        margins[2] = margins[0] + margins[1]

        @pl.when(place == 0)
        def _():
            margins[3] = jnp.zeros_like(margins[3])
            margins[5] = margins[2]
            margin_copy(1, 5, 3, me + 2).start()

        @pl.when(place == chips - 1)
        def _():
            margins[4] = jnp.zeros_like(margins[4])
            margins[6] = margins[2]
            margin_copy(2, 6, 4, me - 2).start()

    def pass_margins():
        @pl.when(place > 0)
        def _():
            margin_copy(1, 5, 3, me - 2).wait_recv()
            margins[5] = margins[2] + margins[3]

        @pl.when(middle)
        def _():
            margin_copy(1, 5, 3, me + 2).start()

        @pl.when(place < chips - 1)
        def _():
            margin_copy(2, 6, 4, me + 2).wait_recv()
            margins[6] = margins[2] + margins[4]

        @pl.when(middle)
        def _():
            margin_copy(2, 6, 4, me - 2).start()

    def own_column(kind):
        lane = lax.broadcasted_iota(jnp.int32, (rows, TILE), 1)
        row = lax.broadcasted_iota(jnp.int32, (rows, TILE), 0)
        column = jnp.zeros((rows, 1), jnp.float32)
        for piece in range(margins.shape[1] - tiles):
            whole = (
                margins[5, tiles + piece, kind : kind + 1, :]
                + margins[4, tiles + piece, kind : kind + 1, :]
            )
            hit = lane + piece * TILE == me * rows + row
            column = column + jnp.sum(jnp.where(hit, whole, 0.0), axis=1, keepdims=True)
        return column

    def finish(tile):
        own[tile, :, place, core] = chip_part(tile, place)

        @pl.when(place > 0)
        def _():
            hop_copy(tile, place, place, me - 2).wait_recv()
            own[tile, :, place, core] = own[tile, :, place, core] + arrived[tile, place]

        @pl.when(place < chips - 1)
        def _():
            hop_copy(tile, place, chips, me + 2).wait_recv()
            own[tile, :, place, core] = own[tile, :, place, core] + arrived[tile, chips]

        sums = own[tile, :, place, core]
        dos_sum, dos_sq = own_column(0), own_column(1)
        gene_sum, gene_sq = (
            margins[5, tile, kind : kind + 1, :] + margins[4, tile, kind : kind + 1, :]
            for kind in (0, 1)
        )
        dosage_var = dos_sq - dos_sum * dos_sum / sample_count
        gene_var = gene_sq - gene_sum * gene_sum / sample_count
        covariance = sums[0] - dos_sum * gene_sum / sample_count
        columns = pl.ds(pl.multiple_of(tile * TILE, TILE), TILE)
        z_total_ref[:, columns] = (
            math.sqrt(sample_count)
            * covariance
            / jnp.sqrt((dosage_var + 1.0) * (gene_var + 1.0))
        )
        z_allelic_ref[:, columns] = sums[1] / jnp.sqrt(sums[2] + 1.0)

    for copy in fetch(0, 0):
        copy.wait()
    if tiles > 1:
        for copy in fetch(1, 1):
            copy.start()
    compute_features(0, 0)
    local.wait()
    for shift in range(1, owners):
        word_copy(shift).wait()
    build_tables()
    multiply(0)
    swap_copy(0).start()

    def compute_step(tile, carry):
        slot = lax.rem(tile, 2)
        for copy in fetch(tile, slot):
            copy.wait()

        @pl.when(tile + 1 < tiles)
        def _():
            for copy in fetch(tile + 1, 1 - slot):
                copy.start()

        compute_features(tile, slot)
        multiply(tile)
        swap_copy(tile).start()

        @pl.when(jnp.logical_and(jnp.logical_not(middle), tile <= meet))
        def _():
            forward(tile - 1)

        @pl.when(jnp.logical_and(middle, jnp.logical_and(lax.rem(tile, 3) == 0, tile <= 3 * early)))
        def _():
            forward(lax.div(tile, 3) - 1)

        return carry

    def forward_step(tile, carry):
        forward(tile)
        return carry

    def finish_step(tile, carry):
        finish(tile)
        return carry

    def later_step(tile, carry):
        @pl.when(middle)
        def _():
            forward(tile)

        finish(tile - 1)
        return carry

    def drain_step(tile, carry):
        drain(tile)
        return carry

    lax.fori_loop(1, tiles, compute_step, 0)
    start_margins()
    lax.fori_loop(jnp.where(middle, early, meet), jnp.where(middle, meet + 1, tiles), forward_step, 0)
    pass_margins()
    lax.fori_loop(0, meet, finish_step, 0)
    lax.fori_loop(meet + 1, tiles, later_step, 0)
    finish(tiles - 1)
    lax.fori_loop(0, tiles, drain_step, 0)
    margin_copy(0, 0, 1, partner).wait_send()

    @pl.when(place < chips - 1)
    def _():
        margin_copy(1, 5, 3, partner).wait_send()

    @pl.when(place > 0)
    def _():
        margin_copy(2, 6, 4, partner).wait_send()


def per_device(hap_words, total_counts, allele_one, allele_two):
    devices = lax.axis_size("samp")
    owners = lax.axis_size("var")
    chips = devices // 2
    samples, genes = total_counts.shape
    _, word_rows, block = hap_words.shape
    variants = block * owners
    rows = variants // devices
    tiles = genes // TILE
    pieces = variants // TILE
    hbm = pl.BlockSpec(memory_space=pltpu.MemorySpace.HBM)
    vmem = pl.BlockSpec(memory_space=pltpu.MemorySpace.VMEM)
    out = jax.ShapeDtypeStruct((rows, genes), jnp.float32)
    dma = pltpu.SemaphoreType.DMA
    f32 = jnp.float32
    return pl.pallas_call(
        functools.partial(kernel, chips, owners),
        out_shape=(out, out),
        in_specs=[hbm] * 4,
        out_specs=(vmem, vmem),
        scratch_shapes=[
            pltpu.VMEM((owners, 2, word_rows, block), jnp.int32),
            pltpu.VMEM((2, samples, block), f32),
            pltpu.VMEM((3, variants, samples), jnp.bfloat16),
            pltpu.VMEM((2, 3, samples, TILE), jnp.int32),
            pltpu.VMEM((3, samples, TILE), jnp.bfloat16),
            pltpu.VMEM((tiles, 3, chips, 2, rows, TILE), f32),
            pltpu.VMEM((tiles, 3, chips, rows, TILE), f32),
            pltpu.VMEM((tiles, chips + 1, 3, rows, TILE), f32),
            pltpu.VMEM((7, tiles + pieces, 2, TILE), f32),
            dma((owners,)),
            dma((owners,)),
            dma,
            dma((2, 3)),
            dma((tiles,)),
            dma((tiles,)),
            dma((tiles, chips)),
            dma((tiles, chips + 1)),
            dma((3,)),
            dma((3,)),
        ],
        compiler_params=pltpu.CompilerParams(
            collective_id=0, has_side_effects=True, vmem_limit_bytes=67043328
        ),
    )(hap_words, total_counts, allele_one, allele_two)


def solution(mesh):
    in_specs = (P(None, "samp", "var"), P("samp", "var"), P("samp", "var"), P("samp", "var"))
    out_specs = (P("samp", "var"), P("samp", "var"))
    return jax.shard_map(
        per_device, mesh=mesh, in_specs=in_specs, out_specs=out_specs, check_vma=False
    )
```

```python
import functools
import math

import jax
import jax.numpy as jnp
from jax import lax
from jax.experimental import pallas as pl
from jax.experimental.pallas import tpu as pltpu
from jax.sharding import PartitionSpec as P

BITS = 30
TILE = 256
CHUNK = 128
MESH = pl.DeviceIdType.MESH


def kernel(
    chips,
    owners,
    hap_ref,
    total_ref,
    one_ref,
    two_ref,
    z_total_ref,
    z_allelic_ref,
    words,
    nat,
    tables,
    inputs,
    feats,
    own,
    swapped,
    arrived,
    results,
    returned,
    margins,
    word_send,
    word_recv,
    word_local,
    in_sem,
    swap_send,
    swap_recv,
    hop_send,
    hop_recv,
    back_send,
    back_recv,
    margin_send,
    margin_recv,
):
    me = lax.axis_index("samp")
    group = lax.axis_index("var")
    place = lax.div(me, 2)
    core = lax.rem(me, 2)
    partner = me + 1 - 2 * core
    word_rows, block = words.shape[2], words.shape[3]
    samples = tables.shape[2]
    tiles = own.shape[0]
    rows = own.shape[4]
    sample_count = float(samples * 2 * chips)
    middle = jnp.logical_and(place > 0, place < chips - 1)
    left_half = place < chips // 2
    meet = max(tiles // 2, 1)

    def fetch(tile, slot):
        columns = pl.ds(pl.multiple_of(tile * TILE, TILE), TILE)
        return [
            pltpu.make_async_copy(
                ref.at[:, columns], inputs.at[slot, kind], in_sem.at[slot, kind]
            )
            for kind, ref in enumerate((total_ref, one_ref, two_ref))
        ]

    for copy in fetch(0, 0):
        copy.start()
    local = pltpu.make_async_copy(hap_ref, words.at[group], word_local)
    local.start()

    barrier = pltpu.get_barrier_semaphore()
    pl.semaphore_signal(barrier, inc=1, device_id={"samp": partner}, device_id_type=MESH)

    @pl.when(place > 0)
    def _():
        pl.semaphore_signal(barrier, inc=1, device_id={"samp": me - 2}, device_id_type=MESH)

    @pl.when(place < chips - 1)
    def _():
        pl.semaphore_signal(barrier, inc=1, device_id={"samp": me + 2}, device_id_type=MESH)

    for far in range(2, chips // 2):
        for toward in (2 * far, -2 * far):
            near_end = place == (0 if toward > 0 else chips - 1)
            from_end = place == (far if toward < 0 else chips - 1 - far)

            @pl.when(jnp.logical_or(near_end, from_end))
            def _():
                pl.semaphore_signal(
                    barrier, inc=1, device_id={"samp": me + toward}, device_id_type=MESH
                )

    for shift in range(1, owners):
        other = lax.rem(group + shift, owners)
        pl.semaphore_signal(barrier, inc=1, device_id={"var": other}, device_id_type=MESH)
    inner = jnp.logical_and(place >= 2, place < chips - 2)
    greeted = jnp.where(middle, jnp.where(inner, 2, 1), chips // 2 - 2)
    pl.semaphore_wait(barrier, owners + 1 + greeted)
    local.wait()

    def peer(shift):
        other = group
        for bit in (1 << place_of for place_of in range(owners.bit_length())):
            if shift & bit:
                other = other + bit - 2 * bit * lax.rem(lax.div(group, bit), 2)
        return other

    def word_copy(shift):
        return pltpu.make_async_remote_copy(
            src_ref=words.at[group],
            dst_ref=words.at[group],
            send_sem=word_send.at[shift],
            recv_sem=word_recv.at[shift],
            device_id={"var": peer(shift)},
            device_id_type=MESH,
        )

    direct = [shift for shift in range(1, owners) if shift & (shift - 1) == 0]
    routed = [shift for shift in range(1, owners) if shift & (shift - 1) != 0]
    for shift in direct:
        word_copy(shift).start()

    def kinds(which):
        return pl.ds(which, 1 + which)

    def swap_copy(tile, which):
        return pltpu.make_async_remote_copy(
            src_ref=own.at[tile, kinds(which), :, 1 - core],
            dst_ref=swapped.at[tile, kinds(which)],
            send_sem=swap_send.at[tile, which],
            recv_sem=swap_recv.at[tile, which],
            device_id={"samp": partner},
            device_id_type=MESH,
        )

    def hop_copy(tile, target, slot, toward, which):
        return pltpu.make_async_remote_copy(
            src_ref=arrived.at[tile, target, kinds(which)],
            dst_ref=arrived.at[tile, slot, kinds(which)],
            send_sem=hop_send.at[tile, target, which],
            recv_sem=hop_recv.at[tile, slot, which],
            device_id={"samp": toward},
            device_id_type=MESH,
        )

    def back_copy(tile, step, target):
        return pltpu.make_async_remote_copy(
            src_ref=results.at[tile, step],
            dst_ref=returned.at[tile],
            send_sem=back_send.at[tile, step],
            recv_sem=back_recv.at[tile],
            device_id={"samp": 2 * target + core},
            device_id_type=MESH,
        )

    def compute_features(tile, slot):
        def step(index, sums):
            part = pl.ds(pl.multiple_of(index * CHUNK, CHUNK), CHUNK)
            log_total = jnp.log(inputs[slot, 0, part, :].astype(jnp.float32) + 1.0)
            feats[0, part, :] = log_total.astype(jnp.bfloat16)
            one = inputs[slot, 1, part, :].astype(jnp.float32) + 1.0
            two = inputs[slot, 2, part, :].astype(jnp.float32) + 1.0
            weight = (one * two) / (one + two)
            ratio = jnp.log(one) - jnp.log(two)
            feats[1, part, :] = (weight * ratio).astype(jnp.bfloat16)
            feats[2, part, :] = weight.astype(jnp.bfloat16)
            split = log_total.reshape(CHUNK // 8, 8, TILE)
            return (sums[0] + jnp.sum(split, axis=0), sums[1] + jnp.sum(split * split, axis=0))

        zero = jnp.zeros((8, TILE), jnp.float32)
        sums = lax.fori_loop(0, samples // CHUNK, step, (zero, zero))
        margins[0, tile, 0:1, :] = jnp.sum(sums[0], axis=0, keepdims=True)
        margins[0, tile, 1:2, :] = jnp.sum(sums[1], axis=0, keepdims=True)

    def build_table(owner):
        first, second = words[owner, 0], words[owner, 1]
        for bit in range(BITS):
            low = jnp.bitwise_and(jnp.right_shift(first, bit), 1)
            high = jnp.bitwise_and(jnp.right_shift(second, bit), 1)
            spread = pl.ds(bit, word_rows, stride=BITS)
            nat[0, spread, :] = (low + high - 1).astype(jnp.float32)
            nat[1, spread, :] = (low - high).astype(jnp.float32)
        dosage = nat[0].T
        phase = nat[1].T
        part = pl.ds(pl.multiple_of(owner * block, block), block)
        tables[0, part, :] = dosage.astype(jnp.bfloat16)
        tables[1, part, :] = phase.astype(jnp.bfloat16)
        tables[2, part, :] = (phase * phase).astype(jnp.bfloat16)

    def sum_tables():
        per_tile = TILE // block
        for owner in range(owners):
            first, second = words[owner, 0], words[owner, 1]
            count = lax.population_count(first) + lax.population_count(second)
            differ = lax.population_count(jnp.bitwise_xor(first, second))
            lanes = pl.ds((owner % per_tile) * block, block)
            place_of = tiles + owner // per_tile
            all_bits = float(BITS * word_rows)
            margins[0, place_of, 0:1, lanes] = (
                jnp.sum(count.astype(jnp.float32), axis=0, keepdims=True) - all_bits
            )
            margins[0, place_of, 1:2, lanes] = all_bits - jnp.sum(
                differ.astype(jnp.float32), axis=0, keepdims=True
            )

    def multiply(tile, kind):
        product = jnp.dot(tables[kind], feats[kind], preferred_element_type=jnp.float32)
        own[tile, kind] = product.reshape(chips, 2, rows, TILE)

    def chip_part(tile, target, which):
        return own[tile, kinds(which), target, core] + swapped[tile, kinds(which), target]

    def hop(tile, target, rightward, which, last):
        head = jnp.where(rightward, 0, chips - 1)
        toward = jnp.where(rightward, me + 2, me - 2)
        behind = jnp.where(rightward, me - 2, me + 2)

        @pl.when(place != head)
        def _():
            hop_copy(tile, target, target, behind, which).wait_recv()
            arrived[tile, target, kinds(which)] = arrived[
                tile, target, kinds(which)
            ] + chip_part(tile, target, which)

        @pl.when(place == head)
        def _():
            arrived[tile, target, kinds(which)] = chip_part(tile, target, which)

        hop_copy(tile, target, jnp.where(last, chips, target), toward, which).start()

    def sweep_total(tile, rightward):
        for step in range(chips - 1):
            target = jnp.where(rightward, chips - 1 - step, step)
            ahead = jnp.where(rightward, target - place, place - target)

            @pl.when(ahead > 0)
            def _():
                last = jnp.logical_and(jnp.logical_not(rightward), ahead == 1)
                hop(tile, target, rightward, 0, last)

    def sweep_allelic(tile, rightward):
        sink = jnp.where(rightward, chips - 1, 0)

        @pl.when(place != sink)
        def _():
            for step in range(chips // 2):
                target = jnp.where(rightward, chips // 2 + step, chips // 2 - 1 - step)
                hop(tile, target, rightward, 1, False)

    def near(tile):
        swap_copy(tile, 0).wait_recv()
        swap_copy(tile, 1).wait_recv()
        sweep_allelic(tile, left_half)
        sweep_total(tile, left_half)

    def far(tile):
        sweep_allelic(tile, jnp.logical_not(left_half))
        sweep_total(tile, jnp.logical_not(left_half))

    def first_forward():
        swap_copy(0, 0).wait_recv()
        sweep_total(0, left_half)
        swap_copy(0, 1).wait_recv()
        sweep_allelic(0, left_half)

    def settle(tile):
        columns = pl.ds(pl.multiple_of(tile * TILE, TILE), TILE)
        for step in range(chips // 2):
            target = jnp.where(left_half, chips // 2 - 1 - step, chips // 2 + step)
            behind = jnp.where(left_half, me + 2, me - 2)
            hop_copy(tile, target, target, behind, 1).wait_recv()
            sums = arrived[tile, target, kinds(1)] + chip_part(tile, target, 1)
            value = sums[0] / jnp.sqrt(sums[1] + 1.0)
            if step < chips // 2 - 1:
                results[tile, step] = value
                back_copy(tile, step, target).start()
            else:
                z_allelic_ref[:, columns] = value

    def deliver(tile):
        columns = pl.ds(pl.multiple_of(tile * TILE, TILE), TILE)
        back_copy(tile, 0, place).wait_recv()
        z_allelic_ref[:, columns] = returned[tile]

    def drain(tile):
        for which in range(2):
            swap_copy(tile, which).wait_send()
        for target in range(chips):

            @pl.when(target != place)
            def _():
                hop_copy(tile, target, target, partner, 0).wait_send()

            sent = jnp.logical_or(
                jnp.logical_and(target < chips // 2, place > 0),
                jnp.logical_and(target >= chips // 2, place < chips - 1),
            )

            @pl.when(sent)
            def _():
                hop_copy(tile, target, target, partner, 1).wait_send()

        @pl.when(jnp.logical_not(middle))
        def _():
            for step in range(chips // 2 - 1):
                back_copy(tile, step, place).wait_send()

    def margin_copy(index, source, slot, toward):
        return pltpu.make_async_remote_copy(
            src_ref=margins.at[source],
            dst_ref=margins.at[slot],
            send_sem=margin_send.at[index],
            recv_sem=margin_recv.at[index],
            device_id={"samp": toward},
            device_id_type=MESH,
        )

    def start_margins():
        margin_copy(0, 0, 1, partner).start()
        margin_copy(0, 0, 1, partner).wait_recv()
        margins[2] = margins[0] + margins[1]

        @pl.when(place == 0)
        def _():
            margins[3] = jnp.zeros_like(margins[3])
            margins[5] = margins[2]
            margin_copy(1, 5, 3, me + 2).start()

        @pl.when(place == chips - 1)
        def _():
            margins[4] = jnp.zeros_like(margins[4])
            margins[6] = margins[2]
            margin_copy(2, 6, 4, me - 2).start()

    def pass_margins(rightward):
        @pl.when(jnp.logical_and(rightward, place > 0))
        def _():
            margin_copy(1, 5, 3, me - 2).wait_recv()
            margins[5] = margins[2] + margins[3]

            @pl.when(middle)
            def _():
                margin_copy(1, 5, 3, me + 2).start()

        @pl.when(jnp.logical_and(jnp.logical_not(rightward), place < chips - 1))
        def _():
            margin_copy(2, 6, 4, me + 2).wait_recv()
            margins[6] = margins[2] + margins[4]

            @pl.when(middle)
            def _():
                margin_copy(2, 6, 4, me - 2).start()

    def own_column(kind):
        lane = lax.broadcasted_iota(jnp.int32, (rows, TILE), 1)
        row = lax.broadcasted_iota(jnp.int32, (rows, TILE), 0)
        column = jnp.zeros((rows, 1), jnp.float32)
        for piece in range(margins.shape[1] - tiles):
            whole = (
                margins[5, tiles + piece, kind : kind + 1, :]
                + margins[4, tiles + piece, kind : kind + 1, :]
            )
            hit = lane + piece * TILE == me * rows + row
            column = column + jnp.sum(jnp.where(hit, whole, 0.0), axis=1, keepdims=True)
        return column

    def finish(tile):
        own[tile, kinds(0), place, core] = chip_part(tile, place, 0)

        @pl.when(place > 0)
        def _():
            hop_copy(tile, place, place, me - 2, 0).wait_recv()
            own[tile, 0, place, core] = own[tile, 0, place, core] + arrived[tile, place, 0]

        @pl.when(place < chips - 1)
        def _():
            hop_copy(tile, place, chips, me + 2, 0).wait_recv()
            own[tile, 0, place, core] = own[tile, 0, place, core] + arrived[tile, chips, 0]

        cross_total = own[tile, 0, place, core]
        dos_sum, dos_sq = own_column(0), own_column(1)
        gene_sum, gene_sq = (
            margins[5, tile, kind : kind + 1, :] + margins[4, tile, kind : kind + 1, :]
            for kind in (0, 1)
        )
        dosage_var = dos_sq - dos_sum * dos_sum / sample_count
        gene_var = gene_sq - gene_sum * gene_sum / sample_count
        covariance = cross_total - dos_sum * gene_sum / sample_count
        columns = pl.ds(pl.multiple_of(tile * TILE, TILE), TILE)
        z_total_ref[:, columns] = (
            math.sqrt(sample_count)
            * covariance
            / jnp.sqrt((dosage_var + 1.0) * (gene_var + 1.0))
        )

    for shift in direct:
        word_copy(shift).wait_send()
    for shift in routed:
        word_copy(shift).start()
    for copy in fetch(0, 0):
        copy.wait()
    if tiles > 1:
        for copy in fetch(1, 1):
            copy.start()
    compute_features(0, 0)
    build_table(group)
    for shift in direct + routed:
        word_copy(shift).wait_recv()
        build_table(peer(shift))
    for shift in routed:
        word_copy(shift).wait_send()
    multiply(0, 0)
    swap_copy(0, 0).start()
    for kind in (1, 2):
        multiply(0, kind)
    swap_copy(0, 1).start()

    @pl.when(jnp.logical_not(middle))
    def _():
        first_forward()

    sum_tables()

    early = 2 if tiles >= 8 else 0
    plan = ((3, near, 0), (5, far, 0), (6, near, 1), (7, far, 1))[: 2 * early]

    def compute_step(tile, carry):
        slot = lax.rem(tile, 2)
        for copy in fetch(tile, slot):
            copy.wait()

        @pl.when(tile + 1 < tiles)
        def _():
            for copy in fetch(tile + 1, 1 - slot):
                copy.start()

        compute_features(tile, slot)
        for kind in range(3):
            multiply(tile, kind)
        for which in range(2):
            swap_copy(tile, which).start()

        @pl.when(jnp.logical_and(jnp.logical_not(middle), jnp.logical_and(tile > 1, tile <= meet)))
        def _():
            near(tile - 1)

        for due, sweep, which in plan:

            @pl.when(jnp.logical_and(middle, tile == due))
            def _():
                sweep(which)

        return carry

    def near_step(tile, carry):
        near(tile)
        return carry

    def both_step(tile, carry):
        near(tile)
        far(tile)
        return carry

    def settle_step(tile, carry):
        @pl.when(jnp.logical_not(middle))
        def _():
            settle(tile)

        return carry

    def finish_step(tile, carry):
        finish(tile)
        return carry

    def later_step(tile, carry):
        @pl.when(jnp.logical_and(middle, tile < tiles))
        def _():
            near(tile)
            far(tile)

        settle_step(tile - 1, 0)
        finish(tile - 1)
        return carry

    def deliver_step(tile, carry):
        deliver(tile)
        return carry

    def drain_step(tile, carry):
        drain(tile)
        return carry

    lax.fori_loop(1, tiles, compute_step, 0)
    start_margins()
    lax.fori_loop(meet, jnp.where(middle, meet, tiles), near_step, 0)
    lax.fori_loop(early, jnp.where(middle, meet + 1, early), both_step, 0)

    @pl.when(middle)
    def _():
        pass_margins(left_half)
        near(meet + 1)
        far(meet + 1)
        pass_margins(jnp.logical_not(left_half))

    lax.fori_loop(0, meet, settle_step, 0)

    @pl.when(jnp.logical_not(middle))
    def _():
        settle(meet)
        pass_margins(jnp.logical_not(left_half))

    lax.fori_loop(0, meet + 1, finish_step, 0)
    lax.fori_loop(meet + 2, tiles + 1, later_step, 0)
    lax.fori_loop(0, jnp.where(middle, tiles, 0), deliver_step, 0)
    lax.fori_loop(0, tiles, drain_step, 0)
    margin_copy(0, 0, 1, partner).wait_send()

    @pl.when(place < chips - 1)
    def _():
        margin_copy(1, 5, 3, partner).wait_send()

    @pl.when(place > 0)
    def _():
        margin_copy(2, 6, 4, partner).wait_send()


def per_device(hap_words, total_counts, allele_one, allele_two):
    devices = lax.axis_size("samp")
    owners = lax.axis_size("var")
    chips = devices // 2
    samples, genes = total_counts.shape
    _, word_rows, block = hap_words.shape
    variants = block * owners
    rows = variants // devices
    tiles = genes // TILE
    pieces = variants // TILE
    hbm = pl.BlockSpec(memory_space=pltpu.MemorySpace.HBM)
    vmem = pl.BlockSpec(memory_space=pltpu.MemorySpace.VMEM)
    out = jax.ShapeDtypeStruct((rows, genes), jnp.float32)
    dma = pltpu.SemaphoreType.DMA
    f32 = jnp.float32
    return pl.pallas_call(
        functools.partial(kernel, chips, owners),
        out_shape=(out, out),
        in_specs=[hbm] * 4,
        out_specs=(vmem, vmem),
        scratch_shapes=[
            pltpu.VMEM((owners, 2, word_rows, block), jnp.int32),
            pltpu.VMEM((2, samples, block), f32),
            pltpu.VMEM((3, variants, samples), jnp.bfloat16),
            pltpu.VMEM((2, 3, samples, TILE), jnp.int32),
            pltpu.VMEM((3, samples, TILE), jnp.bfloat16),
            pltpu.VMEM((tiles, 3, chips, 2, rows, TILE), f32),
            pltpu.VMEM((tiles, 3, chips, rows, TILE), f32),
            pltpu.VMEM((tiles, chips + 1, 3, rows, TILE), f32),
            pltpu.VMEM((tiles, max(chips // 2 - 1, 1), rows, TILE), f32),
            pltpu.VMEM((tiles, rows, TILE), f32),
            pltpu.VMEM((7, tiles + pieces, 2, TILE), f32),
            dma((owners,)),
            dma((owners,)),
            dma,
            dma((2, 3)),
            dma((tiles, 2)),
            dma((tiles, 2)),
            dma((tiles, chips, 2)),
            dma((tiles, chips + 1, 2)),
            dma((tiles, max(chips // 2 - 1, 1))),
            dma((tiles,)),
            dma((3,)),
            dma((3,)),
        ],
        compiler_params=pltpu.CompilerParams(
            collective_id=0, has_side_effects=True, vmem_limit_bytes=67043328
        ),
    )(hap_words, total_counts, allele_one, allele_two)


def solution(mesh):
    in_specs = (P(None, "samp", "var"), P("samp", "var"), P("samp", "var"), P("samp", "var"))
    out_specs = (P("samp", "var"), P("samp", "var"))
    return jax.shard_map(
        per_device, mesh=mesh, in_specs=in_specs, out_specs=out_specs, check_vma=False
    )
```

```python
import functools
import math

import jax
import jax.numpy as jnp
from jax import lax
from jax.experimental import pallas as pl
from jax.experimental.pallas import tpu as pltpu
from jax.sharding import PartitionSpec as P

BITS = 30
TILE = 256
CHUNK = 128
MESH = pl.DeviceIdType.MESH


def kernel(
    chips,
    owners,
    hap_ref,
    total_ref,
    one_ref,
    two_ref,
    z_total_ref,
    z_allelic_ref,
    words,
    nat,
    tables,
    inputs,
    feats,
    own,
    swapped,
    arrived,
    results,
    returned,
    margins,
    word_send,
    word_recv,
    word_local,
    in_sem,
    swap_send,
    swap_recv,
    hop_send,
    hop_recv,
    back_send,
    back_recv,
    margin_send,
    margin_recv,
):
    me = lax.axis_index("samp")
    group = lax.axis_index("var")
    place = lax.div(me, 2)
    core = lax.rem(me, 2)
    partner = me + 1 - 2 * core
    word_rows, block = words.shape[2], words.shape[3]
    samples = tables.shape[2]
    tiles = own.shape[0]
    rows = own.shape[4]
    sample_count = float(samples * 2 * chips)
    middle = jnp.logical_and(place > 0, place < chips - 1)
    left_half = place < chips // 2
    meet = max(tiles // 2, 1)

    def fetch(tile, slot):
        columns = pl.ds(pl.multiple_of(tile * TILE, TILE), TILE)
        return [
            pltpu.make_async_copy(
                ref.at[:, columns], inputs.at[slot, kind], in_sem.at[slot, kind]
            )
            for kind, ref in enumerate((total_ref, one_ref, two_ref))
        ]

    for copy in fetch(0, 0):
        copy.start()
    local = pltpu.make_async_copy(hap_ref, words.at[group], word_local)
    local.start()

    barrier = pltpu.get_barrier_semaphore()
    pl.semaphore_signal(barrier, inc=1, device_id={"samp": partner}, device_id_type=MESH)

    @pl.when(place > 0)
    def _():
        pl.semaphore_signal(barrier, inc=1, device_id={"samp": me - 2}, device_id_type=MESH)

    @pl.when(place < chips - 1)
    def _():
        pl.semaphore_signal(barrier, inc=1, device_id={"samp": me + 2}, device_id_type=MESH)

    for far in range(2, chips // 2):
        for toward in (2 * far, -2 * far):
            near_end = place == (0 if toward > 0 else chips - 1)
            from_end = place == (far if toward < 0 else chips - 1 - far)

            @pl.when(jnp.logical_or(near_end, from_end))
            def _():
                pl.semaphore_signal(
                    barrier, inc=1, device_id={"samp": me + toward}, device_id_type=MESH
                )

    for shift in range(1, owners):
        other = lax.rem(group + shift, owners)
        pl.semaphore_signal(barrier, inc=1, device_id={"var": other}, device_id_type=MESH)
    inner = jnp.logical_and(place >= 2, place < chips - 2)
    greeted = jnp.where(middle, jnp.where(inner, 2, 1), chips // 2 - 2)
    pl.semaphore_wait(barrier, owners + 1 + greeted)
    local.wait()

    def peer(shift):
        other = group
        for bit in (1 << place_of for place_of in range(owners.bit_length())):
            if shift & bit:
                other = other + bit - 2 * bit * lax.rem(lax.div(group, bit), 2)
        return other

    def word_copy(shift):
        return pltpu.make_async_remote_copy(
            src_ref=words.at[group],
            dst_ref=words.at[group],
            send_sem=word_send.at[shift],
            recv_sem=word_recv.at[shift],
            device_id={"var": peer(shift)},
            device_id_type=MESH,
        )

    direct = [shift for shift in range(1, owners) if shift & (shift - 1) == 0]
    routed = [shift for shift in range(1, owners) if shift & (shift - 1) != 0]
    for shift in direct:
        word_copy(shift).start()

    def kinds(which):
        return pl.ds(which, 1 + which)

    def swap_copy(tile, which):
        return pltpu.make_async_remote_copy(
            src_ref=own.at[tile, kinds(which), :, 1 - core],
            dst_ref=swapped.at[tile, kinds(which)],
            send_sem=swap_send.at[tile, which],
            recv_sem=swap_recv.at[tile, which],
            device_id={"samp": partner},
            device_id_type=MESH,
        )

    def hop_copy(tile, target, slot, toward, which):
        return pltpu.make_async_remote_copy(
            src_ref=arrived.at[tile, target, kinds(which)],
            dst_ref=arrived.at[tile, slot, kinds(which)],
            send_sem=hop_send.at[tile, target, which],
            recv_sem=hop_recv.at[tile, slot, which],
            device_id={"samp": toward},
            device_id_type=MESH,
        )

    def back_copy(tile, step, target):
        return pltpu.make_async_remote_copy(
            src_ref=results.at[tile, step],
            dst_ref=returned.at[tile],
            send_sem=back_send.at[tile, step],
            recv_sem=back_recv.at[tile],
            device_id={"samp": 2 * target + core},
            device_id_type=MESH,
        )

    def compute_features(tile, slot):
        def step(index, sums):
            part = pl.ds(pl.multiple_of(index * CHUNK, CHUNK), CHUNK)
            log_total = jnp.log(inputs[slot, 0, part, :].astype(jnp.float32) + 1.0)
            feats[0, part, :] = log_total.astype(jnp.bfloat16)
            one = inputs[slot, 1, part, :].astype(jnp.float32) + 1.0
            two = inputs[slot, 2, part, :].astype(jnp.float32) + 1.0
            weight = (one * two) / (one + two)
            ratio = jnp.log(one) - jnp.log(two)
            feats[1, part, :] = (weight * ratio).astype(jnp.bfloat16)
            feats[2, part, :] = weight.astype(jnp.bfloat16)
            split = log_total.reshape(CHUNK // 8, 8, TILE)
            return (sums[0] + jnp.sum(split, axis=0), sums[1] + jnp.sum(split * split, axis=0))

        zero = jnp.zeros((8, TILE), jnp.float32)
        sums = lax.fori_loop(0, samples // CHUNK, step, (zero, zero))
        margins[0, tile, 0:1, :] = jnp.sum(sums[0], axis=0, keepdims=True)
        margins[0, tile, 1:2, :] = jnp.sum(sums[1], axis=0, keepdims=True)

    def build_table(owner):
        first, second = words[owner, 0], words[owner, 1]
        for bit in range(BITS):
            low = jnp.bitwise_and(jnp.right_shift(first, bit), 1)
            high = jnp.bitwise_and(jnp.right_shift(second, bit), 1)
            spread = pl.ds(bit, word_rows, stride=BITS)
            nat[0, spread, :] = (low + high - 1).astype(jnp.float32)
            nat[1, spread, :] = (low - high).astype(jnp.float32)
        dosage = nat[0].T
        phase = nat[1].T
        part = pl.ds(pl.multiple_of(owner * block, block), block)
        tables[0, part, :] = dosage.astype(jnp.bfloat16)
        tables[1, part, :] = phase.astype(jnp.bfloat16)
        tables[2, part, :] = (phase * phase).astype(jnp.bfloat16)

    def sum_tables():
        per_tile = TILE // block
        for owner in range(owners):
            first, second = words[owner, 0], words[owner, 1]
            count = lax.population_count(first) + lax.population_count(second)
            differ = lax.population_count(jnp.bitwise_xor(first, second))
            lanes = pl.ds((owner % per_tile) * block, block)
            place_of = tiles + owner // per_tile
            all_bits = float(BITS * word_rows)
            margins[0, place_of, 0:1, lanes] = (
                jnp.sum(count.astype(jnp.float32), axis=0, keepdims=True) - all_bits
            )
            margins[0, place_of, 1:2, lanes] = all_bits - jnp.sum(
                differ.astype(jnp.float32), axis=0, keepdims=True
            )

    def multiply(tile, kind):
        product = jnp.dot(tables[kind], feats[kind], preferred_element_type=jnp.float32)
        own[tile, kind] = product.reshape(chips, 2, rows, TILE)

    def chip_part(tile, target, which):
        return own[tile, kinds(which), target, core] + swapped[tile, kinds(which), target]

    def hop(tile, target, rightward, which, last):
        head = jnp.where(rightward, 0, chips - 1)
        toward = jnp.where(rightward, me + 2, me - 2)
        behind = jnp.where(rightward, me - 2, me + 2)

        @pl.when(place != head)
        def _():
            hop_copy(tile, target, target, behind, which).wait_recv()
            arrived[tile, target, kinds(which)] = arrived[
                tile, target, kinds(which)
            ] + chip_part(tile, target, which)

        @pl.when(place == head)
        def _():
            arrived[tile, target, kinds(which)] = chip_part(tile, target, which)

        hop_copy(tile, target, jnp.where(last, chips, target), toward, which).start()

    def hop_total(tile, rightward, step):
        target = jnp.where(rightward, chips - 1 - step, step)
        ahead = jnp.where(rightward, target - place, place - target)

        @pl.when(ahead > 0)
        def _():
            last = jnp.logical_and(jnp.logical_not(rightward), ahead == 1)
            hop(tile, target, rightward, 0, last)

    def hop_allelic(tile, rightward, step):
        sink = jnp.where(rightward, chips - 1, 0)
        target = jnp.where(rightward, chips // 2 + step, chips // 2 - 1 - step)

        @pl.when(place != sink)
        def _():
            hop(tile, target, rightward, 1, False)

    steps = [(hop_allelic, step) for step in range(chips // 2)]
    steps += [(hop_total, step) for step in range(chips - 1)]

    def sweep_total(tile, rightward):
        for step in range(chips - 1):
            hop_total(tile, rightward, step)

    def sweep_allelic(tile, rightward):
        for step in range(chips // 2):
            hop_allelic(tile, rightward, step)

    def near(tile):
        swap_copy(tile, 0).wait_recv()
        swap_copy(tile, 1).wait_recv()
        sweep_allelic(tile, left_half)
        sweep_total(tile, left_half)

    def near_and_far(ahead, behind):
        swap_copy(ahead, 0).wait_recv()
        swap_copy(ahead, 1).wait_recv()
        for one_hop, step in steps:
            one_hop(ahead, left_half, step)
            one_hop(behind, jnp.logical_not(left_half), step)

    def far(tile):
        sweep_allelic(tile, jnp.logical_not(left_half))
        sweep_total(tile, jnp.logical_not(left_half))

    def first_forward():
        swap_copy(0, 0).wait_recv()
        sweep_total(0, left_half)
        swap_copy(0, 1).wait_recv()
        sweep_allelic(0, left_half)

    def settle(tile, send):
        columns = pl.ds(pl.multiple_of(tile * TILE, TILE), TILE)
        for step in range(chips // 2):
            target = jnp.where(left_half, chips // 2 - 1 - step, chips // 2 + step)
            behind = jnp.where(left_half, me + 2, me - 2)
            hop_copy(tile, target, target, behind, 1).wait_recv()
            sums = arrived[tile, target, kinds(1)] + chip_part(tile, target, 1)
            value = sums[0] / jnp.sqrt(sums[1] + 1.0)
            if step < chips // 2 - 1:
                results[tile, step] = value
                if send:
                    back_copy(tile, step, target).start()
            else:
                z_allelic_ref[:, columns] = value

    def send_back(tile):
        for step in range(chips // 2 - 1):
            target = jnp.where(left_half, chips // 2 - 1 - step, chips // 2 + step)
            back_copy(tile, step, target).start()

    def deliver(tile):
        columns = pl.ds(pl.multiple_of(tile * TILE, TILE), TILE)
        back_copy(tile, 0, place).wait_recv()
        z_allelic_ref[:, columns] = returned[tile]

    def drain_hops(tile):
        for which in range(2):
            swap_copy(tile, which).wait_send()
        for target in range(chips):

            @pl.when(target != place)
            def _():
                hop_copy(tile, target, target, partner, 0).wait_send()

            sent = jnp.logical_or(
                jnp.logical_and(target < chips // 2, place > 0),
                jnp.logical_and(target >= chips // 2, place < chips - 1),
            )

            @pl.when(sent)
            def _():
                hop_copy(tile, target, target, partner, 1).wait_send()

    def drain_back(tile):
        for step in range(chips // 2 - 1):
            back_copy(tile, step, place).wait_send()

    def margin_copy(index, source, slot, toward):
        return pltpu.make_async_remote_copy(
            src_ref=margins.at[source],
            dst_ref=margins.at[slot],
            send_sem=margin_send.at[index],
            recv_sem=margin_recv.at[index],
            device_id={"samp": toward},
            device_id_type=MESH,
        )

    def start_margins():
        margin_copy(0, 0, 1, partner).start()
        margin_copy(0, 0, 1, partner).wait_recv()
        margins[2] = margins[0] + margins[1]

        @pl.when(place == 0)
        def _():
            margins[3] = jnp.zeros_like(margins[3])
            margins[5] = margins[2]
            margin_copy(1, 5, 3, me + 2).start()

        @pl.when(place == chips - 1)
        def _():
            margins[4] = jnp.zeros_like(margins[4])
            margins[6] = margins[2]
            margin_copy(2, 6, 4, me - 2).start()

    def pass_margins(rightward):
        @pl.when(jnp.logical_and(rightward, place > 0))
        def _():
            margin_copy(1, 5, 3, me - 2).wait_recv()
            margins[5] = margins[2] + margins[3]

            @pl.when(middle)
            def _():
                margin_copy(1, 5, 3, me + 2).start()

        @pl.when(jnp.logical_and(jnp.logical_not(rightward), place < chips - 1))
        def _():
            margin_copy(2, 6, 4, me + 2).wait_recv()
            margins[6] = margins[2] + margins[4]

            @pl.when(middle)
            def _():
                margin_copy(2, 6, 4, me - 2).start()

    def own_column(kind):
        lane = lax.broadcasted_iota(jnp.int32, (rows, TILE), 1)
        row = lax.broadcasted_iota(jnp.int32, (rows, TILE), 0)
        column = jnp.zeros((rows, 1), jnp.float32)
        for piece in range(margins.shape[1] - tiles):
            whole = (
                margins[5, tiles + piece, kind : kind + 1, :]
                + margins[4, tiles + piece, kind : kind + 1, :]
            )
            hit = lane + piece * TILE == me * rows + row
            column = column + jnp.sum(jnp.where(hit, whole, 0.0), axis=1, keepdims=True)
        return column

    def finish(tile):
        own[tile, kinds(0), place, core] = chip_part(tile, place, 0)

        @pl.when(place > 0)
        def _():
            hop_copy(tile, place, place, me - 2, 0).wait_recv()
            own[tile, 0, place, core] = own[tile, 0, place, core] + arrived[tile, place, 0]

        @pl.when(place < chips - 1)
        def _():
            hop_copy(tile, place, chips, me + 2, 0).wait_recv()
            own[tile, 0, place, core] = own[tile, 0, place, core] + arrived[tile, chips, 0]

        cross_total = own[tile, 0, place, core]
        dos_sum, dos_sq = own_column(0), own_column(1)
        gene_sum, gene_sq = (
            margins[5, tile, kind : kind + 1, :] + margins[4, tile, kind : kind + 1, :]
            for kind in (0, 1)
        )
        dosage_var = dos_sq - dos_sum * dos_sum / sample_count
        gene_var = gene_sq - gene_sum * gene_sum / sample_count
        covariance = cross_total - dos_sum * gene_sum / sample_count
        columns = pl.ds(pl.multiple_of(tile * TILE, TILE), TILE)
        z_total_ref[:, columns] = (
            math.sqrt(sample_count)
            * covariance
            / jnp.sqrt((dosage_var + 1.0) * (gene_var + 1.0))
        )

    for shift in direct:
        word_copy(shift).wait_send()
    for shift in routed:
        word_copy(shift).start()
    for copy in fetch(0, 0):
        copy.wait()
    if tiles > 1:
        for copy in fetch(1, 1):
            copy.start()
    compute_features(0, 0)
    build_table(group)
    for shift in direct + routed:
        word_copy(shift).wait_recv()
        build_table(peer(shift))
    for shift in routed:
        word_copy(shift).wait_send()
    multiply(0, 0)
    swap_copy(0, 0).start()
    for kind in (1, 2):
        multiply(0, kind)
    swap_copy(0, 1).start()

    @pl.when(jnp.logical_not(middle))
    def _():
        first_forward()

    sum_tables()

    early = 2 if tiles >= 8 else 0
    plan = ((3, near, 0), (5, near, 1), (6, far, 0)) if early else ()

    def compute_step(tile, carry):
        slot = lax.rem(tile, 2)
        for copy in fetch(tile, slot):
            copy.wait()

        @pl.when(tile + 1 < tiles)
        def _():
            for copy in fetch(tile + 1, 1 - slot):
                copy.start()

        compute_features(tile, slot)
        for kind in range(3):
            multiply(tile, kind)
        for which in range(2):
            swap_copy(tile, which).start()

        @pl.when(jnp.logical_and(jnp.logical_not(middle), jnp.logical_and(tile > 1, tile <= meet)))
        def _():
            near(tile - 1)

        for due, sweep, which in plan:

            @pl.when(jnp.logical_and(middle, tile == due))
            def _():
                sweep(which)

        return carry

    def near_step(tile, carry):
        near(tile)
        return carry

    def both_step(tile, carry):
        near_and_far(tile, tile - 1)
        return carry

    def settle_step(tile, carry):
        settle(tile, False)
        return carry

    def finish_step(tile, carry):
        finish(tile)
        return carry

    def inner_step(tile, carry):
        near_and_far(tile, tile - 1)
        finish(tile - 1)
        return carry

    def deliver_step(tile, carry):
        deliver(tile)
        return carry

    def hops_step(tile, carry):
        drain_hops(tile)
        return carry

    def send_step(tile, carry):
        send_back(tile)
        return carry

    def back_step(tile, carry):
        drain_back(tile)
        return carry

    lax.fori_loop(1, tiles, compute_step, 0)
    start_margins()
    lax.fori_loop(meet, jnp.where(middle, meet, tiles), near_step, 0)
    if not early:

        @pl.when(middle)
        def _():
            near(0)

    first = max(early, 1)
    lax.fori_loop(first, jnp.where(middle, meet + 1, first), both_step, 0)

    @pl.when(middle)
    def _():
        pass_margins(left_half)
        near_and_far(meet + 1, meet)
        pass_margins(jnp.logical_not(left_half))

        lax.fori_loop(0, meet + 1, finish_step, 0)
        lax.fori_loop(meet + 2, tiles, inner_step, 0)
        far(tiles - 1)
        finish(tiles - 1)
        lax.fori_loop(0, tiles, deliver_step, 0)
        lax.fori_loop(0, tiles, hops_step, 0)

    @pl.when(jnp.logical_not(middle))
    def _():
        lax.fori_loop(0, meet + 1, settle_step, 0)
        pass_margins(jnp.logical_not(left_half))
        lax.fori_loop(0, meet + 1, finish_step, 0)
        held = max(tiles - 2, meet + 1)
        lax.fori_loop(meet + 1, held, settle_step, 0)
        lax.fori_loop(0, tiles, hops_step, 0)
        lax.fori_loop(0, held, send_step, 0)
        for tile in range(held, tiles):
            settle(tile, True)
        lax.fori_loop(meet + 1, tiles, finish_step, 0)
        lax.fori_loop(0, tiles, back_step, 0)

    margin_copy(0, 0, 1, partner).wait_send()

    @pl.when(place < chips - 1)
    def _():
        margin_copy(1, 5, 3, partner).wait_send()

    @pl.when(place > 0)
    def _():
        margin_copy(2, 6, 4, partner).wait_send()


def per_device(hap_words, total_counts, allele_one, allele_two):
    devices = lax.axis_size("samp")
    owners = lax.axis_size("var")
    chips = devices // 2
    samples, genes = total_counts.shape
    _, word_rows, block = hap_words.shape
    variants = block * owners
    rows = variants // devices
    tiles = genes // TILE
    pieces = variants // TILE
    hbm = pl.BlockSpec(memory_space=pltpu.MemorySpace.HBM)
    vmem = pl.BlockSpec(memory_space=pltpu.MemorySpace.VMEM)
    held = pltpu.VMEM((rows, genes), jnp.float32)
    dma = pltpu.SemaphoreType.DMA
    f32 = jnp.float32
    return pl.pallas_call(
        functools.partial(kernel, chips, owners),
        out_shape=(held, held),
        in_specs=[hbm] * 4,
        out_specs=(vmem, vmem),
        scratch_shapes=[
            pltpu.VMEM((owners, 2, word_rows, block), jnp.int32),
            pltpu.VMEM((2, samples, block), f32),
            pltpu.VMEM((3, variants, samples), jnp.bfloat16),
            pltpu.VMEM((2, 3, samples, TILE), jnp.int32),
            pltpu.VMEM((3, samples, TILE), jnp.bfloat16),
            pltpu.VMEM((tiles, 3, chips, 2, rows, TILE), f32),
            pltpu.VMEM((tiles, 3, chips, rows, TILE), f32),
            pltpu.VMEM((tiles, chips + 1, 3, rows, TILE), f32),
            pltpu.VMEM((tiles, max(chips // 2 - 1, 1), rows, TILE), f32),
            pltpu.VMEM((tiles, rows, TILE), f32),
            pltpu.VMEM((7, tiles + pieces, 2, TILE), f32),
            dma((owners,)),
            dma((owners,)),
            dma,
            dma((2, 3)),
            dma((tiles, 2)),
            dma((tiles, 2)),
            dma((tiles, chips, 2)),
            dma((tiles, chips + 1, 2)),
            dma((tiles, max(chips // 2 - 1, 1))),
            dma((tiles,)),
            dma((3,)),
            dma((3,)),
        ],
        compiler_params=pltpu.CompilerParams(
            collective_id=0, has_side_effects=True, vmem_limit_bytes=61 * 2**20
        ),
    )(hap_words, total_counts, allele_one, allele_two)


def solution(mesh):
    in_specs = (P(None, "samp", "var"), P("samp", "var"), P("samp", "var"), P("samp", "var"))
    out_specs = (P("samp", "var"), P("samp", "var"))
    return jax.shard_map(
        per_device, mesh=mesh, in_specs=in_specs, out_specs=out_specs, check_vma=False
    )
```

```python
import functools
import math

import jax
import jax.numpy as jnp
from jax import lax
from jax.experimental import pallas as pl
from jax.experimental.pallas import tpu as pltpu
from jax.sharding import PartitionSpec as P

BITS = 30
TILE = 256
CHUNK = 128
MESH = pl.DeviceIdType.MESH


def kernel(
    chips,
    owners,
    hap_ref,
    total_ref,
    one_ref,
    two_ref,
    z_total_ref,
    z_allelic_ref,
    words,
    nat,
    tables,
    inputs,
    feats,
    own,
    swapped,
    arrived,
    results,
    returned,
    margins,
    word_send,
    word_recv,
    word_local,
    block_send,
    block_recv,
    in_sem,
    swap_send,
    swap_recv,
    hop_send,
    hop_recv,
    back_send,
    back_recv,
    margin_send,
    margin_recv,
):
    me = lax.axis_index("samp")
    group = lax.axis_index("var")
    place = lax.div(me, 2)
    core = lax.rem(me, 2)
    partner = me + 1 - 2 * core
    word_rows, block = words.shape[2], words.shape[3]
    samples = tables.shape[2]
    tiles = own.shape[0]
    rows = own.shape[4]
    sample_count = float(samples * 2 * chips)
    middle = jnp.logical_and(place > 0, place < chips - 1)
    left_half = place < chips // 2
    meet = max(tiles // 2, 1)

    def fetch(tile, slot):
        columns = pl.ds(pl.multiple_of(tile * TILE, TILE), TILE)
        return [
            pltpu.make_async_copy(
                ref.at[:, columns], inputs.at[slot, kind], in_sem.at[slot, kind]
            )
            for kind, ref in enumerate((total_ref, one_ref, two_ref))
        ]

    for copy in fetch(0, 0):
        copy.start()
    local = pltpu.make_async_copy(hap_ref, words.at[group], word_local)
    local.start()

    barrier = pltpu.get_barrier_semaphore()
    pl.semaphore_signal(barrier, inc=1, device_id={"samp": partner}, device_id_type=MESH)

    @pl.when(place > 0)
    def _():
        pl.semaphore_signal(barrier, inc=1, device_id={"samp": me - 2}, device_id_type=MESH)

    @pl.when(place < chips - 1)
    def _():
        pl.semaphore_signal(barrier, inc=1, device_id={"samp": me + 2}, device_id_type=MESH)

    for far in range(2, chips // 2):
        for toward in (2 * far, -2 * far):
            near_end = place == (0 if toward > 0 else chips - 1)
            from_end = place == (far if toward < 0 else chips - 1 - far)

            @pl.when(jnp.logical_or(near_end, from_end))
            def _():
                pl.semaphore_signal(
                    barrier, inc=1, device_id={"samp": me + toward}, device_id_type=MESH
                )

    for shift in range(1, owners):
        other = lax.rem(group + shift, owners)
        pl.semaphore_signal(barrier, inc=1, device_id={"var": other}, device_id_type=MESH)
    inner = jnp.logical_and(place >= 2, place < chips - 2)
    greeted = jnp.where(middle, jnp.where(inner, 2, 1), chips // 2 - 2)

    def peer(shift):
        other = group
        for bit in (1 << place_of for place_of in range(owners.bit_length())):
            if shift & bit:
                other = other + bit - 2 * bit * lax.rem(lax.div(group, bit), 2)
        return other

    def word_copy(shift):
        return pltpu.make_async_remote_copy(
            src_ref=words.at[group],
            dst_ref=words.at[group],
            send_sem=word_send.at[shift],
            recv_sem=word_recv.at[shift],
            device_id={"var": peer(shift)},
            device_id_type=MESH,
        )

    direct = [shift for shift in range(1, owners) if shift & (shift - 1) == 0]
    routed = [shift for shift in range(1, owners) if shift & (shift - 1) != 0]
    def kinds(which):
        return pl.ds(which, 1 + which)

    def swap_copy(tile, which):
        return pltpu.make_async_remote_copy(
            src_ref=own.at[tile, kinds(which), :, 1 - core],
            dst_ref=swapped.at[tile, kinds(which)],
            send_sem=swap_send.at[tile, which],
            recv_sem=swap_recv.at[tile, which],
            device_id={"samp": partner},
            device_id_type=MESH,
        )

    def hop_copy(tile, target, slot, toward, which):
        return pltpu.make_async_remote_copy(
            src_ref=arrived.at[tile, target, kinds(which)],
            dst_ref=arrived.at[tile, slot, kinds(which)],
            send_sem=hop_send.at[tile, target, which],
            recv_sem=hop_recv.at[tile, slot, which],
            device_id={"samp": toward},
            device_id_type=MESH,
        )

    def back_copy(tile, step, target):
        return pltpu.make_async_remote_copy(
            src_ref=results.at[tile, step],
            dst_ref=returned.at[tile],
            send_sem=back_send.at[tile, step],
            recv_sem=back_recv.at[tile],
            device_id={"samp": 2 * target + core},
            device_id_type=MESH,
        )

    def compute_features(tile, slot):
        def step(index, sums):
            part = pl.ds(pl.multiple_of(index * CHUNK, CHUNK), CHUNK)
            log_total = jnp.log(inputs[slot, 0, part, :].astype(jnp.float32) + 1.0)
            feats[0, part, :] = log_total.astype(jnp.bfloat16)
            one = inputs[slot, 1, part, :].astype(jnp.float32) + 1.0
            two = inputs[slot, 2, part, :].astype(jnp.float32) + 1.0
            weight = (one * two) / (one + two)
            ratio = jnp.log(one) - jnp.log(two)
            feats[1, part, :] = (weight * ratio).astype(jnp.bfloat16)
            feats[2, part, :] = weight.astype(jnp.bfloat16)
            split = log_total.reshape(CHUNK // 8, 8, TILE)
            return (sums[0] + jnp.sum(split, axis=0), sums[1] + jnp.sum(split * split, axis=0))

        zero = jnp.zeros((8, TILE), jnp.float32)
        sums = lax.fori_loop(0, samples // CHUNK, step, (zero, zero))
        margins[0, tile, 0:1, :] = jnp.sum(sums[0], axis=0, keepdims=True)
        margins[0, tile, 1:2, :] = jnp.sum(sums[1], axis=0, keepdims=True)

    def build_table(owner):
        first, second = words[owner, 0], words[owner, 1]
        for bit in range(BITS):
            low = jnp.bitwise_and(jnp.right_shift(first, bit), 1)
            high = jnp.bitwise_and(jnp.right_shift(second, bit), 1)
            spread = pl.ds(bit, word_rows, stride=BITS)
            nat[0, spread, :] = (low + high - 1).astype(jnp.float32)
            nat[1, spread, :] = (low - high).astype(jnp.float32)
        dosage = nat[0].T
        phase = nat[1].T
        part = pl.ds(pl.multiple_of(owner * block, block), block)
        tables[0, part, :] = dosage.astype(jnp.bfloat16)
        tables[1, part, :] = phase.astype(jnp.bfloat16)
        tables[2, part, :] = (phase * phase).astype(jnp.bfloat16)

    def sum_tables():
        per_tile = TILE // block
        for owner in range(owners):
            first, second = words[owner, 0], words[owner, 1]
            count = lax.population_count(first) + lax.population_count(second)
            differ = lax.population_count(jnp.bitwise_xor(first, second))
            lanes = pl.ds((owner % per_tile) * block, block)
            place_of = tiles + owner // per_tile
            all_bits = float(BITS * word_rows)
            margins[0, place_of, 0:1, lanes] = (
                jnp.sum(count.astype(jnp.float32), axis=0, keepdims=True) - all_bits
            )
            margins[0, place_of, 1:2, lanes] = all_bits - jnp.sum(
                differ.astype(jnp.float32), axis=0, keepdims=True
            )

    def multiply(tile, kind):
        product = jnp.dot(tables[kind], feats[kind], preferred_element_type=jnp.float32)
        own[tile, kind] = product.reshape(chips, 2, rows, TILE)

    def chip_part(tile, target, which):
        return own[tile, kinds(which), target, core] + swapped[tile, kinds(which), target]

    def hop(tile, target, rightward, which, last):
        head = jnp.where(rightward, 0, chips - 1)
        toward = jnp.where(rightward, me + 2, me - 2)
        behind = jnp.where(rightward, me - 2, me + 2)

        @pl.when(place != head)
        def _():
            hop_copy(tile, target, target, behind, which).wait_recv()
            arrived[tile, target, kinds(which)] = arrived[
                tile, target, kinds(which)
            ] + chip_part(tile, target, which)

        @pl.when(place == head)
        def _():
            arrived[tile, target, kinds(which)] = chip_part(tile, target, which)

        hop_copy(tile, target, jnp.where(last, chips, target), toward, which).start()

    def hop_total(tile, rightward, step):
        target = jnp.where(rightward, chips - 1 - step, step)
        ahead = jnp.where(rightward, target - place, place - target)

        @pl.when(ahead > 0)
        def _():
            last = jnp.logical_and(jnp.logical_not(rightward), ahead == 1)
            hop(tile, target, rightward, 0, last)

    def hop_allelic(tile, rightward, step):
        sink = jnp.where(rightward, chips - 1, 0)
        target = jnp.where(rightward, chips // 2 + step, chips // 2 - 1 - step)

        @pl.when(place != sink)
        def _():
            hop(tile, target, rightward, 1, False)

    steps = [(hop_allelic, step) for step in range(chips // 2)]
    steps += [(hop_total, step) for step in range(chips - 1)]

    def sweep_total(tile, rightward):
        for step in range(chips - 1):
            hop_total(tile, rightward, step)

    def sweep_allelic(tile, rightward):
        for step in range(chips // 2):
            hop_allelic(tile, rightward, step)

    def near(tile):
        if not (isinstance(tile, int) and tile == 0):
            swap_copy(tile, 0).wait_recv()
            swap_copy(tile, 1).wait_recv()
        sweep_allelic(tile, left_half)
        sweep_total(tile, left_half)

    def near_and_far(ahead, behind):
        swap_copy(ahead, 0).wait_recv()
        swap_copy(ahead, 1).wait_recv()
        for one_hop, step in steps:
            one_hop(ahead, left_half, step)
            one_hop(behind, jnp.logical_not(left_half), step)

    def far(tile):
        sweep_allelic(tile, jnp.logical_not(left_half))
        sweep_total(tile, jnp.logical_not(left_half))

    def block_swap(owner, which):
        return pltpu.make_async_remote_copy(
            src_ref=own.at[0, kinds(which), owner, 1 - core],
            dst_ref=swapped.at[0, kinds(which), owner],
            send_sem=block_send.at[owner, which],
            recv_sem=block_recv.at[owner, which],
            device_id={"samp": partner},
            device_id_type=MESH,
        )

    def first_block(owner):
        build_table(owner)
        part = pl.ds(pl.multiple_of(owner * block, block), block)
        for kind in range(3):
            product = jnp.dot(
                tables[kind, part, :], feats[kind], preferred_element_type=jnp.float32
            )
            own[0, kind, owner] = product.reshape(2, rows, TILE)
            if kind != 1:
                block_swap(owner, min(kind, 1)).start()

    def first_hop(target, which):
        block_swap(target, which).wait_recv()
        ahead = jnp.where(left_half, target - place, place - target)
        needed = jnp.where(left_half, target >= chips // 2, target < chips // 2)
        last = jnp.logical_and(jnp.logical_not(left_half), ahead == 1)

        @pl.when(needed if which else ahead > 0)
        def _():
            hop(0, target, left_half, which, False if which else last)

    def settle(tile, send):
        columns = pl.ds(pl.multiple_of(tile * TILE, TILE), TILE)
        for step in range(chips // 2):
            target = jnp.where(left_half, chips // 2 - 1 - step, chips // 2 + step)
            behind = jnp.where(left_half, me + 2, me - 2)
            hop_copy(tile, target, target, behind, 1).wait_recv()
            sums = arrived[tile, target, kinds(1)] + chip_part(tile, target, 1)
            value = sums[0] / jnp.sqrt(sums[1] + 1.0)
            if step < chips // 2 - 1:
                results[tile, step] = value
                if send:
                    back_copy(tile, step, target).start()
            else:
                z_allelic_ref[:, columns] = value

    def send_back(tile):
        for step in range(chips // 2 - 1):
            target = jnp.where(left_half, chips // 2 - 1 - step, chips // 2 + step)
            back_copy(tile, step, target).start()

    def deliver(tile):
        columns = pl.ds(pl.multiple_of(tile * TILE, TILE), TILE)
        back_copy(tile, 0, place).wait_recv()
        z_allelic_ref[:, columns] = returned[tile]

    def drain_hops(tile):
        for which in range(2):

            @pl.when(tile > 0)
            def _():
                swap_copy(tile, which).wait_send()

        for target in range(chips):

            @pl.when(target != place)
            def _():
                hop_copy(tile, target, target, partner, 0).wait_send()

            sent = jnp.logical_or(
                jnp.logical_and(target < chips // 2, place > 0),
                jnp.logical_and(target >= chips // 2, place < chips - 1),
            )

            @pl.when(sent)
            def _():
                hop_copy(tile, target, target, partner, 1).wait_send()

    def drain_back(tile):
        for step in range(chips // 2 - 1):
            back_copy(tile, step, place).wait_send()

    def margin_copy(index, source, slot, toward):
        return pltpu.make_async_remote_copy(
            src_ref=margins.at[source],
            dst_ref=margins.at[slot],
            send_sem=margin_send.at[index],
            recv_sem=margin_recv.at[index],
            device_id={"samp": toward},
            device_id_type=MESH,
        )

    def start_margins():
        margin_copy(0, 0, 1, partner).start()
        margin_copy(0, 0, 1, partner).wait_recv()
        margins[2] = margins[0] + margins[1]

        @pl.when(place == 0)
        def _():
            margins[3] = jnp.zeros_like(margins[3])
            margins[5] = margins[2]
            margin_copy(1, 5, 3, me + 2).start()

        @pl.when(place == chips - 1)
        def _():
            margins[4] = jnp.zeros_like(margins[4])
            margins[6] = margins[2]
            margin_copy(2, 6, 4, me - 2).start()

    def pass_margins(rightward):
        @pl.when(jnp.logical_and(rightward, place > 0))
        def _():
            margin_copy(1, 5, 3, me - 2).wait_recv()
            margins[5] = margins[2] + margins[3]

            @pl.when(middle)
            def _():
                margin_copy(1, 5, 3, me + 2).start()

        @pl.when(jnp.logical_and(jnp.logical_not(rightward), place < chips - 1))
        def _():
            margin_copy(2, 6, 4, me + 2).wait_recv()
            margins[6] = margins[2] + margins[4]

            @pl.when(middle)
            def _():
                margin_copy(2, 6, 4, me - 2).start()

    def own_column(kind):
        lane = lax.broadcasted_iota(jnp.int32, (rows, TILE), 1)
        row = lax.broadcasted_iota(jnp.int32, (rows, TILE), 0)
        column = jnp.zeros((rows, 1), jnp.float32)
        for piece in range(margins.shape[1] - tiles):
            whole = (
                margins[5, tiles + piece, kind : kind + 1, :]
                + margins[4, tiles + piece, kind : kind + 1, :]
            )
            hit = lane + piece * TILE == me * rows + row
            column = column + jnp.sum(jnp.where(hit, whole, 0.0), axis=1, keepdims=True)
        return column

    def finish(tile):
        own[tile, kinds(0), place, core] = chip_part(tile, place, 0)

        @pl.when(place > 0)
        def _():
            hop_copy(tile, place, place, me - 2, 0).wait_recv()
            own[tile, 0, place, core] = own[tile, 0, place, core] + arrived[tile, place, 0]

        @pl.when(place < chips - 1)
        def _():
            hop_copy(tile, place, chips, me + 2, 0).wait_recv()
            own[tile, 0, place, core] = own[tile, 0, place, core] + arrived[tile, chips, 0]

        cross_total = own[tile, 0, place, core]
        dos_sum, dos_sq = own_column(0), own_column(1)
        gene_sum, gene_sq = (
            margins[5, tile, kind : kind + 1, :] + margins[4, tile, kind : kind + 1, :]
            for kind in (0, 1)
        )
        dosage_var = dos_sq - dos_sum * dos_sum / sample_count
        gene_var = gene_sq - gene_sum * gene_sum / sample_count
        covariance = cross_total - dos_sum * gene_sum / sample_count
        columns = pl.ds(pl.multiple_of(tile * TILE, TILE), TILE)
        z_total_ref[:, columns] = (
            math.sqrt(sample_count)
            * covariance
            / jnp.sqrt((dosage_var + 1.0) * (gene_var + 1.0))
        )

    for copy in fetch(0, 0):
        copy.wait()
    if tiles > 1:
        for copy in fetch(1, 1):
            copy.start()
    compute_features(0, 0)
    pl.semaphore_wait(barrier, owners + 1 + greeted)
    local.wait()
    for shift in direct:
        word_copy(shift).start()

    blocks = [0] + direct + routed
    for index, shift in enumerate(blocks):
        if shift:
            word_copy(shift).wait_recv()
        first_block(peer(shift))
        if not shift:
            for other in direct:
                word_copy(other).wait_send()
            for other in routed:
                word_copy(other).start()

        @pl.when(jnp.logical_not(middle))
        def _():
            if index:
                first_hop(peer(blocks[index - 1]), 1)
            first_hop(peer(shift), 0)

    @pl.when(jnp.logical_not(middle))
    def _():
        first_hop(peer(blocks[-1]), 1)

    @pl.when(middle)
    def _():
        for shift in blocks:
            for which in range(2):
                block_swap(peer(shift), which).wait_recv()

    for shift in routed:
        word_copy(shift).wait_send()

    sum_tables()

    early = 2 if tiles >= 8 else 0
    plan = ((3, near, 0), (5, near, 1), (6, far, 0)) if early else ()

    def compute_step(tile, carry):
        slot = lax.rem(tile, 2)
        for copy in fetch(tile, slot):
            copy.wait()

        @pl.when(tile + 1 < tiles)
        def _():
            for copy in fetch(tile + 1, 1 - slot):
                copy.start()

        compute_features(tile, slot)
        for kind in range(3):
            multiply(tile, kind)
        for which in range(2):
            swap_copy(tile, which).start()

        if meet > 1:

            @pl.when(jnp.logical_and(jnp.logical_not(middle), tile == 1))
            def _():
                near(tile)

        @pl.when(jnp.logical_and(jnp.logical_not(middle), jnp.logical_and(tile > 2, tile <= meet)))
        def _():
            near(tile - 1)

        for due, sweep, which in plan:

            @pl.when(jnp.logical_and(middle, tile == due))
            def _():
                sweep(which)

        return carry

    def near_step(tile, carry):
        near(tile)
        return carry

    def both_step(tile, carry):
        near_and_far(tile, tile - 1)
        return carry

    def settle_step(tile, carry):
        settle(tile, False)
        return carry

    def finish_step(tile, carry):
        finish(tile)
        return carry

    def inner_step(tile, carry):
        near_and_far(tile, tile - 1)
        finish(tile - 1)
        return carry

    def deliver_step(tile, carry):
        deliver(tile)
        return carry

    def hops_step(tile, carry):
        drain_hops(tile)
        return carry

    def send_step(tile, carry):
        send_back(tile)
        return carry

    def back_step(tile, carry):
        drain_back(tile)
        return carry

    lax.fori_loop(1, tiles, compute_step, 0)
    start_margins()
    lax.fori_loop(meet, jnp.where(middle, meet, tiles), near_step, 0)
    if not early:

        @pl.when(middle)
        def _():
            near(0)

    first = max(early, 1)
    lax.fori_loop(first, jnp.where(middle, meet + 1, first), both_step, 0)

    @pl.when(middle)
    def _():
        pass_margins(left_half)
        near_and_far(meet + 1, meet)
        pass_margins(jnp.logical_not(left_half))

        lax.fori_loop(0, meet + 1, finish_step, 0)
        lax.fori_loop(meet + 2, tiles, inner_step, 0)
        far(tiles - 1)
        finish(tiles - 1)
        lax.fori_loop(0, tiles, deliver_step, 0)
        lax.fori_loop(0, tiles, hops_step, 0)

    @pl.when(jnp.logical_not(middle))
    def _():
        lax.fori_loop(0, meet + 1, settle_step, 0)
        pass_margins(jnp.logical_not(left_half))
        lax.fori_loop(0, meet + 1, finish_step, 0)
        held = max(tiles - 2, meet + 1)
        lax.fori_loop(meet + 1, held, settle_step, 0)
        lax.fori_loop(0, tiles, hops_step, 0)
        lax.fori_loop(0, held, send_step, 0)
        for tile in range(held, tiles):
            settle(tile, True)
        lax.fori_loop(meet + 1, tiles, finish_step, 0)
        lax.fori_loop(0, tiles, back_step, 0)

    for shift in blocks:
        for which in range(2):
            block_swap(peer(shift), which).wait_send()
    margin_copy(0, 0, 1, partner).wait_send()

    @pl.when(place < chips - 1)
    def _():
        margin_copy(1, 5, 3, partner).wait_send()

    @pl.when(place > 0)
    def _():
        margin_copy(2, 6, 4, partner).wait_send()


def per_device(hap_words, total_counts, allele_one, allele_two):
    devices = lax.axis_size("samp")
    owners = lax.axis_size("var")
    chips = devices // 2
    samples, genes = total_counts.shape
    _, word_rows, block = hap_words.shape
    variants = block * owners
    rows = variants // devices
    tiles = genes // TILE
    pieces = variants // TILE
    hbm = pl.BlockSpec(memory_space=pltpu.MemorySpace.HBM)
    vmem = pl.BlockSpec(memory_space=pltpu.MemorySpace.VMEM)
    held = pltpu.VMEM((rows, genes), jnp.float32)
    dma = pltpu.SemaphoreType.DMA
    f32 = jnp.float32
    return pl.pallas_call(
        functools.partial(kernel, chips, owners),
        out_shape=(held, held),
        in_specs=[hbm] * 4,
        out_specs=(vmem, vmem),
        scratch_shapes=[
            pltpu.VMEM((owners, 2, word_rows, block), jnp.int32),
            pltpu.VMEM((2, samples, block), f32),
            pltpu.VMEM((3, variants, samples), jnp.bfloat16),
            pltpu.VMEM((2, 3, samples, TILE), jnp.int32),
            pltpu.VMEM((3, samples, TILE), jnp.bfloat16),
            pltpu.VMEM((tiles, 3, chips, 2, rows, TILE), f32),
            pltpu.VMEM((tiles, 3, chips, rows, TILE), f32),
            pltpu.VMEM((tiles, chips + 1, 3, rows, TILE), f32),
            pltpu.VMEM((tiles, max(chips // 2 - 1, 1), rows, TILE), f32),
            pltpu.VMEM((tiles, rows, TILE), f32),
            pltpu.VMEM((7, tiles + pieces, 2, TILE), f32),
            dma((owners,)),
            dma((owners,)),
            dma,
            dma((owners, 2)),
            dma((owners, 2)),
            dma((2, 3)),
            dma((tiles, 2)),
            dma((tiles, 2)),
            dma((tiles, chips, 2)),
            dma((tiles, chips + 1, 2)),
            dma((tiles, max(chips // 2 - 1, 1))),
            dma((tiles,)),
            dma((3,)),
            dma((3,)),
        ],
        compiler_params=pltpu.CompilerParams(
            collective_id=0, has_side_effects=True, vmem_limit_bytes=61 * 2**20
        ),
    )(hap_words, total_counts, allele_one, allele_two)


def solution(mesh):
    in_specs = (P(None, "samp", "var"), P("samp", "var"), P("samp", "var"), P("samp", "var"))
    out_specs = (P("samp", "var"), P("samp", "var"))
    return jax.shard_map(
        per_device, mesh=mesh, in_specs=in_specs, out_specs=out_specs, check_vma=False
    )
```
